512 devices in a mesh: beam: 2 (over y), tm: 16 (over z), sect: 8 (over x), pol: 2 (over core).
Axes of the slice: x: 8, y: 2, z: 16, core: 2. Of those that a mesh axis runs over, the one named last changes fastest.
The devices are a block of a 8x8x16 slice.
Arguments:
- signal: float32 [2, 2, 8192, 4096], P(None, 'pol', ('beam', 'tm', 'sect')), parts along dimension 2, may hold values from -6 to 6
- coarse_taps: float32 [16, 4096], replicated, may hold values from -1.5 to 1.5
- fine_taps: float32 [16, 1024], replicated, may hold values from -1.5 to 1.5
- channel_order: int32 [4096], replicated, may hold values from 0 to 4095, each once
Outputs:
- fine_spectra: float32 [2, 2, 8192, 4, 1024], P(None, 'pol', ('beam', 'tm', 'sect')), parts along dimension 2
The draws below stay inside these ranges and needn't reach their ends.
There are 2 independent parts, one for each index of `beam`. The reference program is written for one: setup_inputs(seed, part) draws one part's arguments, and reference() takes and returns one part's arrays. A program takes and returns all parts, laid end to end along the dimension named above; an argument that names none is the same for every part. Nothing has to cross between parts.
Inputs may be any that keep to these rules, and one draw needn't show every extreme that they name: `channel_order`: each of the 4096 coarse channels appears exactly once.
All inputs are finite; a program needn't handle non-finite values.
Results may differ from the reference program's by a relative error of at most 0.0001.
Values sent between devices are 32-bit elements; how exact they have to be, the bound alone decides.
A program may use at most 64 MiB of HBM per device.

```python
import jax
import jax.numpy as jnp
from jax import lax

COARSE = 4096
FINE = 1024
TAPS = 16
POL = 2
TSPEC = 4096
FSPEC = 4


def block_scale(stream_key, shape, split, least, high):
    factor_of, own = 1.0, jax.random.fold_in(stream_key, 6)
    for position, parts in split:
        steps = jnp.exp(jax.random.uniform(jax.random.fold_in(own, position), (parts,), jnp.float32, least / len(split), high / len(split)))
        factor_of = factor_of * jnp.repeat(steps, shape[position] // parts).reshape([-1 if axis == position else 1 for axis in range(len(shape))])
    return factor_of


def gaussian(own_key, extent, width, reach, split=(), kind=jnp.bfloat16):
    gain = block_scale(own_key, extent, split, -0.22, 0.18) if split else 1.0
    result = jax.random.normal(own_key, extent, jnp.float32) * width * gain
    return jnp.minimum(jnp.maximum(result, -reach), reach).astype(kind)


def setup_inputs(seed: int = 0, part: int = 0) -> dict:
    key_of = jax.random.split(jax.random.key(seed), 5)
    part_keys = jax.random.split(jax.random.fold_in(key_of[4], part), 5)
    signal = gaussian(part_keys[0], (2, POL, TSPEC, COARSE), 1.0, 6.0, ((1, 2), (2, 128)), jnp.float32)
    coarse_taps = gaussian(key_of[1], (TAPS, COARSE), TAPS ** -0.5, 1.5, (), jnp.float32)
    fine_taps = gaussian(key_of[2], (TAPS, FINE), TAPS ** -0.5, 1.5, (), jnp.float32)
    channel_order = jax.random.permutation(key_of[3], COARSE).astype(jnp.int32)
    return dict(signal=signal, coarse_taps=coarse_taps, fine_taps=fine_taps, channel_order=channel_order)


def reference(signal, coarse_taps, fine_taps, channel_order):
    frame_count = TSPEC
    results = []
    for polar_index in range(signal.shape[1]):
        complex_slab = lax.complex(signal[0, polar_index], signal[1, polar_index])
        padded = jnp.concatenate([complex_slab, jnp.zeros((TAPS - 1, COARSE), complex_slab.dtype)], axis=0)
        filtered = coarse_taps[0] * padded[0:frame_count]
        for tap_index in range(1, TAPS):
            filtered = filtered + coarse_taps[tap_index] * padded[tap_index:tap_index + frame_count]
        coarse = jnp.fft.fft(filtered, axis=1, norm="ortho")
        series = jnp.take(coarse, channel_order, axis=1).T
        total_len = (FSPEC + TAPS - 1) * FINE
        series = jnp.pad(series, ((0, 0), (0, total_len - frame_count)))
        frames = series.reshape(COARSE, FSPEC + TAPS - 1, FINE)
        fine_filtered = fine_taps[0] * frames[:, 0:FSPEC]
        for tap_index in range(1, TAPS):
            fine_filtered = fine_filtered + fine_taps[tap_index] * frames[:, tap_index:tap_index + FSPEC]
        fine = jnp.fft.fft(fine_filtered, axis=2, norm="ortho")
        results.append(jnp.stack([jnp.real(fine), jnp.imag(fine)]))
    return jnp.stack(results, axis=1).astype(jnp.float32)
```

```python
from functools import partial
import math

import jax
import jax.numpy as jnp
from jax import lax
from jax.experimental import pallas as pl
from jax.experimental.pallas import tpu as pltpu
from jax.sharding import PartitionSpec as P
import ml_dtypes
import numpy as np

LANES = 128
SUB = 8
F32 = jnp.float32
BF16 = jnp.bfloat16


def split_np(table):
    high = table.astype(ml_dtypes.bfloat16)
    low = (table - high.astype(np.float64)).astype(ml_dtypes.bfloat16)
    return high, low


def dft_matrix(size):
    grid = np.outer(np.arange(size), np.arange(size)) % size
    angle = -2.0 * np.pi * grid / size
    cos, sin = np.cos(angle), np.sin(angle)
    return split_np(np.block([[cos, sin], [-sin, cos]]))


def twiddles(rows, cols, period, scale):
    angle = -2.0 * np.pi * (np.outer(np.arange(rows), np.arange(cols)) % period) / period
    return np.stack([np.cos(angle), np.sin(angle)]).astype(np.float32) * np.float32(scale)


def split(value):
    high = value.astype(BF16)
    return high, (value - high.astype(F32)).astype(BF16)


def times(value, re, im):
    return (value[0] * re - value[1] * im, value[0] * im + value[1] * re)


def add(a, b):
    return (a[0] + b[0], a[1] + b[1])


def sub(a, b):
    return (a[0] - b[0], a[1] - b[1])


def minus_i(a):
    return (a[1], -a[0])


def dft4(x):
    s0, d0, s1, d1 = add(x[0], x[2]), sub(x[0], x[2]), add(x[1], x[3]), minus_i(sub(x[1], x[3]))
    return [add(s0, s1), add(d0, d1), sub(s0, s1), sub(d0, d1)]


def dft8(x):
    half = math.sqrt(0.5)
    even, odd = dft4(x[0::2]), dft4(x[1::2])
    o1, o3 = odd[1], odd[3]
    odd = [
        odd[0],
        ((o1[0] + o1[1]) * half, (o1[1] - o1[0]) * half),
        minus_i(odd[2]),
        ((o3[1] - o3[0]) * half, (o3[0] + o3[1]) * -half),
    ]
    return [add(e, o) for e, o in zip(even, odd)] + [sub(e, o) for e, o in zip(even, odd)]


def group_transpose(vecs, lane):
    size = LANES // 4
    vecs = list(vecs)
    for dist in (1, 2):
        keep = (lane // (size * dist)) % 2 == 0
        for i in range(4):
            if i & dist:
                continue
            a, b = vecs[i], vecs[i + dist]
            vecs[i] = jnp.where(keep, a, pltpu.roll(b, size * dist, 1))
            vecs[i + dist] = jnp.where(keep, pltpu.roll(a, LANES - size * dist, 1), b)
    return vecs


def coarse_fft(half, rows, x_scr, taps_ref, tw_ref, wh_ref, wl_ref, u_scr, lh_scr, ll_scr, y_scr):
    tap_count = taps_ref.shape[0]
    cols = x_scr.shape[1]
    fold = cols // 4
    for r in range(fold):
        parts = []
        for q in range(4):
            a = r + fold * q
            acc = [None, None]
            for k in range(tap_count):
                tap = taps_ref[k : k + 1, a * LANES : (a + 1) * LANES]
                for comp in range(2):
                    term = tap * x_scr[comp, a, pl.ds(half * rows + k, rows, 1), :]
                    acc[comp] = term if k == 0 else acc[comp] + term
            parts.append(tuple(acc))
        for k1, value in enumerate(dft4(parts)):
            if r and k1:
                angle = -2.0 * math.pi * r * k1 / cols
                value = times(value, math.cos(angle), math.sin(angle))
            for comp in range(2):
                u_scr[comp, r, k1] = value[comp]
    for k1 in range(4):
        outs = dft8([(u_scr[0, r, k1], u_scr[1, r, k1]) for r in range(fold)])
        for k2, value in enumerate(outs):
            k = k1 + 4 * k2
            value = times(value, tw_ref[0, k : k + 1, :], tw_ref[1, k : k + 1, :])
            for comp in range(2):
                high, low = split(value[comp])
                lh_scr[pl.ds(k * rows, rows), comp * LANES : (comp + 1) * LANES] = high
                ll_scr[pl.ds(k * rows, rows), comp * LANES : (comp + 1) * LANES] = low
    step = 8 * rows
    for base in range(0, cols * rows, step):
        high, low = lh_scr[base : base + step], ll_scr[base : base + step]
        dot = partial(jnp.dot, preferred_element_type=F32)
        out = dot(high, wh_ref[...]) + (dot(low, wh_ref[...]) + dot(high, wl_ref[...]))
        for comp in range(2):
            piece = out[:, comp * LANES : (comp + 1) * LANES]
            y_scr[comp, base // rows : (base + step) // rows] = piece.reshape(8, rows, LANES)


def order_channels(half, order_ref, y_scr, put):
    cols = y_scr.shape[1]
    lane = lax.broadcasted_iota(jnp.int32, (SUB, LANES), 1)

    def step(q, carry):
        chan = jnp.broadcast_to(order_ref[pl.ds(q, 1), :], (SUB, LANES))
        source, which = chan // cols, chan % cols
        accs = [jnp.zeros((SUB, LANES), F32)] * 4
        for k in range(cols):
            mine = which == k
            for u in range(4):
                vec = y_scr[u // 2, k, (u % 2) * SUB : (u % 2 + 1) * SUB, :]
                got = jnp.take_along_axis(vec, source, axis=1, mode="promise_in_bounds")
                accs[u] = jnp.where(mine, got, accs[u])
        for r, vec in enumerate(group_transpose(accs, lane)):
            put(q, r, vec)
        return carry

    lax.fori_loop(0, order_ref.shape[0], step, 0)


def coarse_kernel(sig_ref, halo_ref, taps_ref, order_ref, tw_ref, wh_ref, wl_ref, out_ref,
                  x_scr, u_scr, lh_scr, ll_scr, y_scr, sem):
    slab = sig_ref.shape[2]
    cols = x_scr.shape[1]
    rows = slab // 2
    lead = halo_ref.shape[2]
    copies = []
    for comp in range(2):
        for a in range(cols):
            lanes = pl.ds(a * LANES, LANES)
            copies.append(pltpu.make_async_copy(
                sig_ref.at[comp, 0, :, lanes], x_scr.at[comp, a, pl.ds(0, slab), :], sem.at[0]))
            copies.append(pltpu.make_async_copy(
                halo_ref.at[comp, 0, :, lanes], x_scr.at[comp, a, pl.ds(slab, lead), :], sem.at[0]))
    for copy in copies:
        copy.start()
    for copy in copies:
        copy.wait()
    for half in range(2):
        coarse_fft(half, rows, x_scr, taps_ref, tw_ref, wh_ref, wl_ref, u_scr, lh_scr, ll_scr, y_scr)

        def put(q, r, vec, half=half):
            out_ref[4 * q + r, half] = vec

        order_channels(half, order_ref, y_scr, put)


def fine_fir(arr_ref, taps_ref, xs_scr, frames, per):
    lane = lax.broadcasted_iota(jnp.int32, (SUB, LANES), 1)
    row = lax.broadcasted_iota(jnp.int32, (SUB, LANES), 0)
    slots = LANES // 4
    spread = (lane % 4) * slots + lane // 4
    group = lane // slots
    slab = 4 * SUB

    def step(jb, carry):
        for k4 in range(4):
            jd = jb * 4 + k4
            for half in range(2):
                pick = k4 * slab + half * 2 * SUB + (group % 2) * SUB + row
                taps = [
                    jnp.take_along_axis(
                        jnp.broadcast_to(taps_ref[jb, k : k + 1, :], (SUB, LANES)), pick, axis=1,
                        mode="promise_in_bounds")
                    for k in range(min(frames, taps_ref.shape[1]))
                ]
                data = [arr_ref[g * per + jd, half] for g in range(frames)]
                outs = []
                for f in range(frames):
                    acc = None
                    for k in range(min(frames - f, len(taps))):
                        term = taps[k] * data[f + k]
                        acc = term if acc is None else acc + term
                    outs.append(acc)
                for u, vec in enumerate(group_transpose(outs, lane)):
                    vec = jnp.take_along_axis(vec, spread, axis=1, mode="promise_in_bounds")
                    base = pl.multiple_of(jd * slab + half * 2 * SUB + (u % 2) * SUB, SUB)
                    xs_scr[u // 2, pl.ds(base, SUB), :] = vec
        return carry

    lax.fori_loop(0, per // 4, step, 0)


def fine_fft(xs_scr, tw_ref, wh_ref, wl_ref, p_scr, out_ref):
    fold = xs_scr.shape[1] // LANES
    dot = partial(jnp.dot, preferred_element_type=F32)
    for a in range(fold):
        pieces = [jnp.transpose(xs_scr[comp, pl.ds(a, LANES, fold), :]) for comp in range(2)]
        high, low = split(jnp.concatenate(pieces, axis=1))
        out = dot(high, wh_ref[...]) + (dot(low, wh_ref[...]) + dot(high, wl_ref[...]))
        value = times((out[:, :LANES], out[:, LANES:]), tw_ref[0, a : a + 1, :], tw_ref[1, a : a + 1, :])
        for comp in range(2):
            p_scr[comp, a] = value[comp]
    frames = out_ref.shape[3]
    pack = SUB // frames

    def step(i, carry):
        rows = pl.ds(pl.multiple_of(i * SUB, SUB), SUB)
        outs = dft8([(p_scr[0, a, rows, :], p_scr[1, a, rows, :]) for a in range(fold)])
        for m1, value in enumerate(outs):
            for comp in range(2):
                out_ref[comp, 0, pl.ds(i * pack, pack), :, m1 * LANES : (m1 + 1) * LANES] = value[
                    comp].reshape(pack, frames, LANES)
        return carry

    lax.fori_loop(0, LANES // SUB, step, 0)


def fine_kernel(arr_ref, taps_ref, tw_ref, wh_ref, wl_ref, out_ref, xs_scr, p_scr):
    frames = out_ref.shape[3]
    fine_fir(arr_ref, taps_ref, xs_scr, frames, arr_ref.shape[0] // frames)
    fine_fft(xs_scr, tw_ref, wh_ref, wl_ref, p_scr, out_ref)


def shifted(value, axis, steps):
    count = lax.axis_size(axis)
    return lax.ppermute(value, axis, [(i, i + steps) for i in range(max(0, -steps), min(count, count - steps))])


def tables(width, fine):
    cols, fold = width // LANES, fine // LANES
    wh, wl = dft_matrix(LANES)
    tw_c = twiddles(cols, LANES, width, width ** -0.5)
    tw_f = twiddles(fold, LANES, fine, fine ** -0.5)
    return [jnp.asarray(t) for t in (wh, wl, tw_c, tw_f)]


def run_coarse(signal, halo, coarse_taps, order, wh, wl, tw_c, owners):
    slab, width = signal.shape[2:]
    cols = width // LANES
    rows = slab // 2
    vmem = pl.BlockSpec(memory_space=pltpu.VMEM)
    anym = pl.BlockSpec(memory_space=pl.ANY)
    return pl.pallas_call(
        coarse_kernel,
        out_shape=jax.ShapeDtypeStruct((owners, 2, SUB, LANES), F32),
        in_specs=[anym, anym, vmem, vmem, vmem, vmem, vmem],
        out_specs=vmem,
        scratch_shapes=[
            pltpu.VMEM((2, cols, slab + 16, LANES), F32),
            pltpu.VMEM((2, cols // 4, 4, rows, LANES), F32),
            pltpu.VMEM((cols * rows, 2 * LANES), BF16),
            pltpu.VMEM((cols * rows, 2 * LANES), BF16),
            pltpu.VMEM((2, cols, rows, LANES), F32),
            pltpu.SemaphoreType.DMA((1,)),
        ],
        name="coarse",
    )(signal, halo, coarse_taps, order, tw_c, wh, wl)


def run_fine(arrived, taps, wh, wl, tw_f, own, frames, fine):
    vmem = pl.BlockSpec(memory_space=pltpu.VMEM)
    return pl.pallas_call(
        fine_kernel,
        out_shape=jax.ShapeDtypeStruct((2, 1, own, frames, fine), F32),
        in_specs=[vmem] * 5,
        out_specs=vmem,
        scratch_shapes=[
            pltpu.VMEM((2, fine, LANES), F32),
            pltpu.VMEM((2, fine // LANES, LANES, LANES), F32),
        ],
        name="fine",
    )(arrived, taps, tw_f, wh, wl)


def body(signal, coarse_taps, fine_taps, channel_order):
    _, polars, slab, width = signal.shape
    tap_count, fine = fine_taps.shape
    owners = lax.axis_size(("tm", "sect"))
    own = width // owners
    frames = slab * owners // fine
    assert polars == 1 and slab == 4 * SUB and 4 * own == LANES and frames == 4 and tap_count == 16
    wh, wl, tw_c, tw_f = tables(width, fine)
    halo = shifted(signal[:, :, : tap_count - 1, :], ("tm", "sect"), -1)
    order = channel_order.reshape(width // LANES, LANES)
    blocks = run_coarse(signal, halo, coarse_taps, order, wh, wl, tw_c, owners)
    arrived = lax.all_to_all(blocks, ("tm", "sect"), split_axis=0, concat_axis=0, tiled=True)
    taps = jnp.swapaxes(fine_taps.reshape(tap_count, fine // LANES, LANES), 0, 1)
    return run_fine(arrived, taps, wh, wl, tw_f, own, frames, fine)


def solution(mesh):
    in_specs = (P(None, "pol", ("beam", "tm", "sect"), None), P(), P(), P())
    out_specs = P(None, "pol", ("beam", "tm", "sect"), None, None)
    return jax.shard_map(body, mesh=mesh, in_specs=in_specs, out_specs=out_specs, check_vma=False)
```

```python
from functools import partial
import math

import jax
import jax.numpy as jnp
from jax import lax
from jax.experimental import pallas as pl
from jax.experimental.pallas import tpu as pltpu
from jax.sharding import PartitionSpec as P
import ml_dtypes
import numpy as np

LANES = 128
SUB = 8
F32 = jnp.float32
BF16 = jnp.bfloat16


def split_np(table):
    high = table.astype(ml_dtypes.bfloat16)
    low = (table - high.astype(np.float64)).astype(ml_dtypes.bfloat16)
    return high, low


def dft_matrix(size):
    grid = np.outer(np.arange(size), np.arange(size)) % size
    angle = -2.0 * np.pi * grid / size
    cos, sin = np.cos(angle), np.sin(angle)
    return split_np(np.block([[cos, sin], [-sin, cos]]))


def twiddles(rows, cols, period, scale):
    angle = -2.0 * np.pi * (np.outer(np.arange(rows), np.arange(cols)) % period) / period
    return np.stack([np.cos(angle), np.sin(angle)]).astype(np.float32) * np.float32(scale)


def split(value):
    high = value.astype(BF16)
    return high, (value - high.astype(F32)).astype(BF16)


def times(value, re, im):
    return (value[0] * re - value[1] * im, value[0] * im + value[1] * re)


def add(a, b):
    return (a[0] + b[0], a[1] + b[1])


def sub(a, b):
    return (a[0] - b[0], a[1] - b[1])


def minus_i(a):
    return (a[1], -a[0])


def dft4(x):
    s0, d0, s1, d1 = add(x[0], x[2]), sub(x[0], x[2]), add(x[1], x[3]), minus_i(sub(x[1], x[3]))
    return [add(s0, s1), add(d0, d1), sub(s0, s1), sub(d0, d1)]


def dft8(x):
    half = math.sqrt(0.5)
    even, odd = dft4(x[0::2]), dft4(x[1::2])
    o1, o3 = odd[1], odd[3]
    odd = [
        odd[0],
        ((o1[0] + o1[1]) * half, (o1[1] - o1[0]) * half),
        minus_i(odd[2]),
        ((o3[1] - o3[0]) * half, (o3[0] + o3[1]) * -half),
    ]
    return [add(e, o) for e, o in zip(even, odd)] + [sub(e, o) for e, o in zip(even, odd)]


def group_transpose(vecs, lane):
    size = LANES // 4
    vecs = list(vecs)
    for dist in (1, 2):
        keep = (lane // (size * dist)) % 2 == 0
        for i in range(4):
            if i & dist:
                continue
            a, b = vecs[i], vecs[i + dist]
            vecs[i] = jnp.where(keep, a, pltpu.roll(b, size * dist, 1))
            vecs[i + dist] = jnp.where(keep, pltpu.roll(a, LANES - size * dist, 1), b)
    return vecs


def coarse_fft(half, rows, x_scr, taps_ref, tw_ref, wh_ref, wl_ref, u_scr, lh_scr, ll_scr, y_scr):
    tap_count = taps_ref.shape[0]
    cols = x_scr.shape[1]
    fold = cols // 4
    for r in range(fold):
        parts = []
        for q in range(4):
            a = r + fold * q
            acc = [None, None]
            for k in range(tap_count):
                tap = taps_ref[k : k + 1, a * LANES : (a + 1) * LANES]
                for comp in range(2):
                    term = tap * x_scr[comp, a, pl.ds(half * rows + k, rows, 1), :]
                    acc[comp] = term if k == 0 else acc[comp] + term
            parts.append(tuple(acc))
        for k1, value in enumerate(dft4(parts)):
            if r and k1:
                angle = -2.0 * math.pi * r * k1 / cols
                value = times(value, math.cos(angle), math.sin(angle))
            for comp in range(2):
                u_scr[comp, r, k1] = value[comp]
    for k1 in range(4):
        outs = dft8([(u_scr[0, r, k1], u_scr[1, r, k1]) for r in range(fold)])
        for k2, value in enumerate(outs):
            k = k1 + 4 * k2
            value = times(value, tw_ref[0, k : k + 1, :], tw_ref[1, k : k + 1, :])
            for comp in range(2):
                high, low = split(value[comp])
                lh_scr[pl.ds(k * rows, rows), comp * LANES : (comp + 1) * LANES] = high
                ll_scr[pl.ds(k * rows, rows), comp * LANES : (comp + 1) * LANES] = low
    step = 8 * rows
    for base in range(0, cols * rows, step):
        high, low = lh_scr[base : base + step], ll_scr[base : base + step]
        dot = partial(jnp.dot, preferred_element_type=F32)
        out = dot(high, wh_ref[...]) + (dot(low, wh_ref[...]) + dot(high, wl_ref[...]))
        for comp in range(2):
            piece = out[:, comp * LANES : (comp + 1) * LANES]
            y_scr[comp, base // rows : (base + step) // rows] = piece.reshape(8, rows, LANES)


def order_channels(half, order_ref, y_scr, put):
    cols = y_scr.shape[1]
    lane = lax.broadcasted_iota(jnp.int32, (SUB, LANES), 1)

    def step(q, carry):
        chan = jnp.broadcast_to(order_ref[pl.ds(q, 1), :], (SUB, LANES))
        source, which = chan // cols, chan % cols
        accs = [jnp.zeros((SUB, LANES), F32)] * 4
        for k in range(cols):
            mine = which == k
            for u in range(4):
                vec = y_scr[u // 2, k, (u % 2) * SUB : (u % 2 + 1) * SUB, :]
                got = jnp.take_along_axis(vec, source, axis=1, mode="promise_in_bounds")
                accs[u] = jnp.where(mine, got, accs[u])
        for r, vec in enumerate(group_transpose(accs, lane)):
            put(q, r, vec)
        return carry

    lax.fori_loop(0, order_ref.shape[0], step, 0)


def coarse_kernel(sig_ref, halo_ref, taps_ref, order_ref, tw_ref, wh_ref, wl_ref, out_ref,
                  x_scr, u_scr, lh_scr, ll_scr, y_scr, sem):
    slab = sig_ref.shape[2]
    cols = x_scr.shape[1]
    rows = slab // 2
    lead = halo_ref.shape[2]
    copies = []
    for comp in range(2):
        for a in range(cols):
            lanes = pl.ds(a * LANES, LANES)
            copies.append(pltpu.make_async_copy(
                sig_ref.at[comp, 0, :, lanes], x_scr.at[comp, a, pl.ds(0, slab), :], sem.at[0]))
            copies.append(pltpu.make_async_copy(
                halo_ref.at[comp, 0, :, lanes], x_scr.at[comp, a, pl.ds(slab, lead), :], sem.at[0]))
    for copy in copies:
        copy.start()
    for copy in copies:
        copy.wait()
    for half in range(2):
        coarse_fft(half, rows, x_scr, taps_ref, tw_ref, wh_ref, wl_ref, u_scr, lh_scr, ll_scr, y_scr)

        def put(q, r, vec, half=half):
            sects = out_ref.shape[1]
            owner = 4 * q + r
            out_ref[owner // sects, owner % sects, half] = vec

        order_channels(half, order_ref, y_scr, put)


def fine_fir(arr_ref, taps_ref, xs_scr, frames, per):
    lane = lax.broadcasted_iota(jnp.int32, (SUB, LANES), 1)
    row = lax.broadcasted_iota(jnp.int32, (SUB, LANES), 0)
    slots = LANES // 4
    spread = (lane % 4) * slots + lane // 4
    group = lane // slots
    slab = 4 * SUB

    def step(jb, carry):
        for k4 in range(4):
            jd = jb * 4 + k4
            for half in range(2):
                pick = k4 * slab + half * 2 * SUB + (group % 2) * SUB + row
                taps = [
                    jnp.take_along_axis(
                        jnp.broadcast_to(taps_ref[jb, k : k + 1, :], (SUB, LANES)), pick, axis=1,
                        mode="promise_in_bounds")
                    for k in range(min(frames, taps_ref.shape[1]))
                ]
                data = [arr_ref[g * per + jd, half] for g in range(frames)]
                outs = []
                for f in range(frames):
                    acc = None
                    for k in range(min(frames - f, len(taps))):
                        term = taps[k] * data[f + k]
                        acc = term if acc is None else acc + term
                    outs.append(acc)
                for u, vec in enumerate(group_transpose(outs, lane)):
                    vec = jnp.take_along_axis(vec, spread, axis=1, mode="promise_in_bounds")
                    base = pl.multiple_of(jd * slab + half * 2 * SUB + (u % 2) * SUB, SUB)
                    xs_scr[u // 2, pl.ds(base, SUB), :] = vec
        return carry

    lax.fori_loop(0, per // 4, step, 0)


def fine_fft(xs_scr, tw_ref, wh_ref, wl_ref, p_scr, out_ref):
    fold = xs_scr.shape[1] // LANES
    dot = partial(jnp.dot, preferred_element_type=F32)
    for a in range(fold):
        pieces = [jnp.transpose(xs_scr[comp, pl.ds(a, LANES, fold), :]) for comp in range(2)]
        high, low = split(jnp.concatenate(pieces, axis=1))
        out = dot(high, wh_ref[...]) + (dot(low, wh_ref[...]) + dot(high, wl_ref[...]))
        value = times((out[:, :LANES], out[:, LANES:]), tw_ref[0, a : a + 1, :], tw_ref[1, a : a + 1, :])
        for comp in range(2):
            p_scr[comp, a] = value[comp]
    frames = out_ref.shape[3]
    pack = SUB // frames

    def step(i, carry):
        rows = pl.ds(pl.multiple_of(i * SUB, SUB), SUB)
        outs = dft8([(p_scr[0, a, rows, :], p_scr[1, a, rows, :]) for a in range(fold)])
        for m1, value in enumerate(outs):
            for comp in range(2):
                out_ref[comp, 0, pl.ds(i * pack, pack), :, m1 * LANES : (m1 + 1) * LANES] = value[
                    comp].reshape(pack, frames, LANES)
        return carry

    lax.fori_loop(0, LANES // SUB, step, 0)


def fine_kernel(arr_ref, taps_ref, tw_ref, wh_ref, wl_ref, out_ref, xs_scr, p_scr):
    frames = out_ref.shape[3]
    fine_fir(arr_ref, taps_ref, xs_scr, frames, arr_ref.shape[0] // frames)
    fine_fft(xs_scr, tw_ref, wh_ref, wl_ref, p_scr, out_ref)


LAG = 3


def exchange_kernel(blk_ref, arr_ref, relay, in_sem, below, far_send, far_recv, row_send, row_recv):
    tms, sects = blk_ref.shape[:2]
    x, z = lax.axis_index("sect"), lax.axis_index("tm")
    last = tms - 1
    barrier = pltpu.get_barrier_semaphore()
    mesh_id = pl.DeviceIdType.MESH

    def tell(sem, **where):
        pl.semaphore_signal(sem, inc=1, device_id=where, device_id_type=mesh_id)

    def loop(low, high, step):
        lax.fori_loop(low, high, lambda i, carry: (step(i), carry)[1], 0)

    def spread(source, j):
        def send(i):
            near = i // 2 + 1
            to = lax.rem(x + near + (i % 2) * (sects - 2 * near), sects)
            pltpu.make_async_remote_copy(
                source.at[to], arr_ref.at[j, x], row_send.at[j], row_recv.at[j],
                device_id={"sect": to}, device_id_type=mesh_id).start()

        loop(0, sects - 1, send)
        arr_ref[j, x] = source[x]

    def across(j):
        pltpu.make_async_remote_copy(
            blk_ref.at[j], relay.at[z], far_send.at[j], far_recv.at[z],
            device_id={"tm": j}, device_id_type=mesh_id).start()

    loop(1, sects, lambda i: tell(barrier, sect=lax.rem(x + i, sects)))

    @pl.when(z > 0)
    def _():
        tell(barrier, tm=z - 1)

    pl.semaphore_wait(barrier, sects - 1 + (last - z + last - 1) // last)

    @pl.when(z > 0)
    def _():
        pl.semaphore_wait(below, 1)

    @pl.when(z < last)
    def _():
        tell(below, tm=z + 1)
        loop(0, z, lambda j: tell(in_sem.at[z + 1], tm=j))

    loop(0, z, across)
    spread(blk_ref.at[z], z)

    def step(s):
        @pl.when(s < last - z)
        def _():
            @pl.when(s > 0)
            def _():
                pl.semaphore_wait(in_sem.at[z + 1 + s], 1)

            across(z + 1 + s)

        @pl.when(s >= LAG)
        def _():
            i = s - LAG
            j = i + (i + tms - z) // tms
            pltpu.make_async_copy(relay.at[j], relay.at[j], far_recv.at[j]).wait()
            spread(relay.at[j], j)

    loop(0, last + LAG, step)

    def finish(j):
        part = arr_ref.at[j, pl.ds(0, sects - 1)]
        pltpu.make_async_copy(part, part, row_send.at[j]).wait()
        pltpu.make_async_copy(part, part, row_recv.at[j]).wait()

        @pl.when(j != z)
        def _():
            pltpu.make_async_copy(blk_ref.at[j], blk_ref.at[j], far_send.at[j]).wait()

    loop(0, tms, finish)


def run_exchange(blocks):
    tms = blocks.shape[0]
    vmem = pl.BlockSpec(memory_space=pltpu.VMEM)
    dma = pltpu.SemaphoreType.DMA((tms,))
    return pl.pallas_call(
        exchange_kernel,
        out_shape=jax.ShapeDtypeStruct(blocks.shape, F32),
        in_specs=[vmem],
        out_specs=vmem,
        scratch_shapes=[
            pltpu.VMEM(blocks.shape, F32),
            pltpu.SemaphoreType.REGULAR((tms,)),
            pltpu.SemaphoreType.REGULAR,
            dma, dma, dma, dma,
        ],
        compiler_params=pltpu.CompilerParams(collective_id=0, has_side_effects=True),
        name="exchange",
    )(blocks)


def shifted(value, axis, steps):
    count = lax.axis_size(axis)
    return lax.ppermute(value, axis, [(i, i + steps) for i in range(max(0, -steps), min(count, count - steps))])


def tables(width, fine):
    cols, fold = width // LANES, fine // LANES
    wh, wl = dft_matrix(LANES)
    tw_c = twiddles(cols, LANES, width, width ** -0.5)
    tw_f = twiddles(fold, LANES, fine, fine ** -0.5)
    return [jnp.asarray(t) for t in (wh, wl, tw_c, tw_f)]


def run_coarse(signal, halo, coarse_taps, order, wh, wl, tw_c, sects, tms):
    slab, width = signal.shape[2:]
    cols = width // LANES
    rows = slab // 2
    vmem = pl.BlockSpec(memory_space=pltpu.VMEM)
    anym = pl.BlockSpec(memory_space=pl.ANY)
    return pl.pallas_call(
        coarse_kernel,
        out_shape=jax.ShapeDtypeStruct((tms, sects, 2, SUB, LANES), F32),
        in_specs=[anym, anym, vmem, vmem, vmem, vmem, vmem],
        out_specs=vmem,
        scratch_shapes=[
            pltpu.VMEM((2, cols, slab + 16, LANES), F32),
            pltpu.VMEM((2, cols // 4, 4, rows, LANES), F32),
            pltpu.VMEM((cols * rows, 2 * LANES), BF16),
            pltpu.VMEM((cols * rows, 2 * LANES), BF16),
            pltpu.VMEM((2, cols, rows, LANES), F32),
            pltpu.SemaphoreType.DMA((1,)),
        ],
        name="coarse",
    )(signal, halo, coarse_taps, order, tw_c, wh, wl)


def run_fine(arrived, taps, wh, wl, tw_f, own, frames, fine):
    vmem = pl.BlockSpec(memory_space=pltpu.VMEM)
    return pl.pallas_call(
        fine_kernel,
        out_shape=jax.ShapeDtypeStruct((2, 1, own, frames, fine), F32),
        in_specs=[vmem] * 5,
        out_specs=vmem,
        scratch_shapes=[
            pltpu.VMEM((2, fine, LANES), F32),
            pltpu.VMEM((2, fine // LANES, LANES, LANES), F32),
        ],
        name="fine",
    )(arrived, taps, tw_f, wh, wl)


def body(signal, coarse_taps, fine_taps, channel_order):
    _, polars, slab, width = signal.shape
    tap_count, fine = fine_taps.shape
    owners = lax.axis_size(("tm", "sect"))
    own = width // owners
    frames = slab * owners // fine
    assert polars == 1 and slab == 4 * SUB and 4 * own == LANES and frames == 4 and tap_count == 16
    wh, wl, tw_c, tw_f = tables(width, fine)
    halo = shifted(signal[:, :, : tap_count - 1, :], ("tm", "sect"), -1)
    order = channel_order.reshape(width // LANES, LANES)
    sects, tms = lax.axis_size("sect"), lax.axis_size("tm")
    blocks = run_coarse(signal, halo, coarse_taps, order, wh, wl, tw_c, sects, tms)
    arrived = run_exchange(blocks).reshape(owners, 2, SUB, LANES)
    taps = jnp.swapaxes(fine_taps.reshape(tap_count, fine // LANES, LANES), 0, 1)
    return run_fine(arrived, taps, wh, wl, tw_f, own, frames, fine)


def solution(mesh):
    in_specs = (P(None, "pol", ("beam", "tm", "sect"), None), P(), P(), P())
    out_specs = P(None, "pol", ("beam", "tm", "sect"), None, None)
    return jax.shard_map(body, mesh=mesh, in_specs=in_specs, out_specs=out_specs, check_vma=False)
```

```python
from functools import partial
import math

import jax
import jax.numpy as jnp
from jax import lax
from jax.experimental import pallas as pl
from jax.experimental.pallas import tpu as pltpu
from jax.sharding import PartitionSpec as P
import ml_dtypes
import numpy as np

LANES = 128
SUB = 8
F32 = jnp.float32
BF16 = jnp.bfloat16


def split_np(table):
    high = table.astype(ml_dtypes.bfloat16)
    low = (table - high.astype(np.float64)).astype(ml_dtypes.bfloat16)
    return high, low


def dft_matrix(size):
    grid = np.outer(np.arange(size), np.arange(size)) % size
    angle = -2.0 * np.pi * grid / size
    cos, sin = np.cos(angle), np.sin(angle)
    return split_np(np.block([[cos, sin], [-sin, cos]]))


def twiddles(rows, cols, period, scale):
    angle = -2.0 * np.pi * (np.outer(np.arange(rows), np.arange(cols)) % period) / period
    return np.stack([np.cos(angle), np.sin(angle)]).astype(np.float32) * np.float32(scale)


def split(value):
    high = value.astype(BF16)
    return high, (value - high.astype(F32)).astype(BF16)


def times(value, re, im):
    return (value[0] * re - value[1] * im, value[0] * im + value[1] * re)


def add(a, b):
    return (a[0] + b[0], a[1] + b[1])


def sub(a, b):
    return (a[0] - b[0], a[1] - b[1])


def minus_i(a):
    return (a[1], -a[0])


def dft4(x):
    s0, d0, s1, d1 = add(x[0], x[2]), sub(x[0], x[2]), add(x[1], x[3]), minus_i(sub(x[1], x[3]))
    return [add(s0, s1), add(d0, d1), sub(s0, s1), sub(d0, d1)]


def dft8(x):
    half = math.sqrt(0.5)
    even, odd = dft4(x[0::2]), dft4(x[1::2])
    o1, o3 = odd[1], odd[3]
    odd = [
        odd[0],
        ((o1[0] + o1[1]) * half, (o1[1] - o1[0]) * half),
        minus_i(odd[2]),
        ((o3[1] - o3[0]) * half, (o3[0] + o3[1]) * -half),
    ]
    return [add(e, o) for e, o in zip(even, odd)] + [sub(e, o) for e, o in zip(even, odd)]


def group_transpose(vecs, lane):
    size = LANES // 4
    vecs = list(vecs)
    for dist in (1, 2):
        keep = (lane // (size * dist)) % 2 == 0
        for i in range(4):
            if i & dist:
                continue
            a, b = vecs[i], vecs[i + dist]
            vecs[i] = jnp.where(keep, a, pltpu.roll(b, size * dist, 1))
            vecs[i + dist] = jnp.where(keep, pltpu.roll(a, LANES - size * dist, 1), b)
    return vecs


def coarse_fft(half, rows, x_scr, taps_ref, tw_ref, wh_ref, wl_ref, u_scr, lh_scr, ll_scr, y_scr):
    tap_count = taps_ref.shape[0]
    cols = x_scr.shape[1]
    fold = cols // 4
    for r in range(fold):
        parts = []
        for q in range(4):
            a = r + fold * q
            acc = [None, None]
            for k in range(tap_count):
                tap = taps_ref[k : k + 1, a * LANES : (a + 1) * LANES]
                for comp in range(2):
                    term = tap * x_scr[comp, a, pl.ds(half * rows + k, rows, 1), :]
                    acc[comp] = term if k == 0 else acc[comp] + term
            parts.append(tuple(acc))
        for k1, value in enumerate(dft4(parts)):
            if r and k1:
                angle = -2.0 * math.pi * r * k1 / cols
                value = times(value, math.cos(angle), math.sin(angle))
            for comp in range(2):
                u_scr[comp, r, k1] = value[comp]
    for k1 in range(4):
        outs = dft8([(u_scr[0, r, k1], u_scr[1, r, k1]) for r in range(fold)])
        for k2, value in enumerate(outs):
            k = k1 + 4 * k2
            value = times(value, tw_ref[0, k : k + 1, :], tw_ref[1, k : k + 1, :])
            for comp in range(2):
                high, low = split(value[comp])
                lh_scr[pl.ds(k * rows, rows), comp * LANES : (comp + 1) * LANES] = high
                ll_scr[pl.ds(k * rows, rows), comp * LANES : (comp + 1) * LANES] = low
    step = 8 * rows
    for base in range(0, cols * rows, step):
        high, low = lh_scr[base : base + step], ll_scr[base : base + step]
        dot = partial(jnp.dot, preferred_element_type=F32)
        out = dot(high, wh_ref[...]) + (dot(low, wh_ref[...]) + dot(high, wl_ref[...]))
        for comp in range(2):
            piece = out[:, comp * LANES : (comp + 1) * LANES]
            y_scr[comp, base // rows : (base + step) // rows] = piece.reshape(8, rows, LANES)


def order_channels(index_ref, y_scr, z_scr, g_scr, put):
    cols, rows = y_scr.shape[1:3]
    lane = lax.broadcasted_iota(jnp.int32, (SUB, LANES), 1)
    for k in range(cols):
        both = jnp.concatenate([y_scr[0, k], y_scr[1, k]], axis=0)
        z_scr[k * LANES : (k + 1) * LANES, :] = jnp.transpose(jnp.concatenate([both] * 4, axis=0))
    row_lane = lax.broadcasted_iota(jnp.int32, (1, LANES), 1)
    group = LANES // 4
    chunk = 16

    def step(part, carry):
        def fetch(i, inner):
            for u in range(chunk):
                at = i * chunk + u
                got = [z_scr[pl.ds(index_ref[(part * 4 + h) * LANES + at], 1), :] for h in range(4)]
                low = jnp.where(row_lane < group, got[0], got[1])
                high = jnp.where(row_lane < 3 * group, got[2], got[3])
                g_scr[pl.ds(at, 1), :] = jnp.where(row_lane < 2 * group, low, high)
            return inner

        lax.fori_loop(0, LANES // chunk, fetch, 0)
        turned = jnp.transpose(g_scr[...])
        for h in range(4):
            vecs = [turned[(h * 4 + u) * SUB : (h * 4 + u + 1) * SUB] for u in range(4)]
            for r, vec in enumerate(group_transpose(vecs, lane)):
                put(part * 4 + h, r, vec)
        return carry

    lax.fori_loop(0, cols // 4, step, 0)


def fine_fir(arr_ref, taps_ref, xs_scr, frames, per):
    lane = lax.broadcasted_iota(jnp.int32, (SUB, LANES), 1)
    row = lax.broadcasted_iota(jnp.int32, (SUB, LANES), 0)
    slots = LANES // 4
    spread = (lane % 4) * slots + lane // 4
    group = lane // slots
    slab = 4 * SUB

    def step(jb, carry):
        for k4 in range(4):
            jd = jb * 4 + k4
            for half in range(2):
                pick = k4 * slab + half * 2 * SUB + (group % 2) * SUB + row
                taps = [
                    jnp.take_along_axis(
                        jnp.broadcast_to(taps_ref[jb, k : k + 1, :], (SUB, LANES)), pick, axis=1,
                        mode="promise_in_bounds")
                    for k in range(min(frames, taps_ref.shape[1]))
                ]
                data = [arr_ref[half, g * per + jd] for g in range(frames)]
                outs = []
                for f in range(frames):
                    acc = None
                    for k in range(min(frames - f, len(taps))):
                        term = taps[k] * data[f + k]
                        acc = term if acc is None else acc + term
                    outs.append(acc)
                for u, vec in enumerate(group_transpose(outs, lane)):
                    vec = jnp.take_along_axis(vec, spread, axis=1, mode="promise_in_bounds")
                    base = pl.multiple_of(jd * slab + half * 2 * SUB + (u % 2) * SUB, SUB)
                    xs_scr[u // 2, pl.ds(base, SUB), :] = vec
        return carry

    lax.fori_loop(0, per // 4, step, 0)


def fine_fft(xs_scr, tw_ref, wh_ref, wl_ref, p_scr, out_ref):
    fold = xs_scr.shape[1] // LANES
    dot = partial(jnp.dot, preferred_element_type=F32)
    for a in range(fold):
        pieces = [jnp.transpose(xs_scr[comp, pl.ds(a, LANES, fold), :]) for comp in range(2)]
        high, low = split(jnp.concatenate(pieces, axis=1))
        out = dot(high, wh_ref[...]) + (dot(low, wh_ref[...]) + dot(high, wl_ref[...]))
        value = times((out[:, :LANES], out[:, LANES:]), tw_ref[0, a : a + 1, :], tw_ref[1, a : a + 1, :])
        for comp in range(2):
            p_scr[comp, a] = value[comp]
    frames = out_ref.shape[3]
    pack = SUB // frames

    def step(i, carry):
        rows = pl.ds(pl.multiple_of(i * SUB, SUB), SUB)
        outs = dft8([(p_scr[0, a, rows, :], p_scr[1, a, rows, :]) for a in range(fold)])
        for m1, value in enumerate(outs):
            for comp in range(2):
                out_ref[comp, 0, pl.ds(i * pack, pack), :, m1 * LANES : (m1 + 1) * LANES] = value[
                    comp].reshape(pack, frames, LANES)
        return carry

    lax.fori_loop(0, LANES // SUB, step, 0)


def fine_kernel(arr_ref, taps_ref, tw_ref, wh_ref, wl_ref, out_ref, xs_scr, p_scr):
    frames = out_ref.shape[3]
    fine_fir(arr_ref, taps_ref, xs_scr, frames, arr_ref.shape[1] // frames)
    fine_fft(xs_scr, tw_ref, wh_ref, wl_ref, p_scr, out_ref)


LAG = 3


def front_kernel(sig_ref, taps_ref, index_ref, tw_ref, wh_ref, wl_ref, arr_ref,
                 x_scr, halo, u_scr, lh_scr, ll_scr, y_scr, z_scr, g_scr, blk, relay,
                 load_sem, halo_sem, in_sem, below, far_send, far_recv, row_send, row_recv):
    slab = sig_ref.shape[2]
    cols = x_scr.shape[1]
    rows = slab // 2
    lead = halo.shape[1]
    tms, sects = blk.shape[1:3]
    x, z = lax.axis_index("sect"), lax.axis_index("tm")
    last, edge = tms - 1, sects - 1
    barrier = pltpu.get_barrier_semaphore()
    mesh_id = pl.DeviceIdType.MESH

    def tell(sem, **where):
        pl.semaphore_signal(sem, inc=1, device_id=where, device_id_type=mesh_id)

    def loop(low, high, step):
        lax.fori_loop(low, high, lambda i, carry: (step(i), carry)[1], 0)

    def load(a):
        lanes = pl.ds(pl.multiple_of(a * LANES, LANES), LANES)
        for comp in range(2):
            pltpu.make_async_copy(
                sig_ref.at[comp, 0, :, lanes], x_scr.at[comp, a, pl.ds(0, slab), :], load_sem).start()

    loop(0, cols, load)

    loop(1, sects, lambda i: tell(barrier, sect=lax.rem(x + i, sects)))

    @pl.when(z > 0)
    def _():
        tell(barrier, tm=z - 1)

    @pl.when(jnp.logical_and(x == edge, z < last))
    def _():
        tell(barrier, tm=z + 1, sect=0)

    not_last = (last - z + last - 1) // last
    wraps = (1 - (x + edge) // sects) * ((z + last - 1) // last)
    has_next = z * sects + x < tms * sects - 1

    def halo_copy():
        return pltpu.make_async_remote_copy(
            sig_ref.at[:, 0, pl.ds(0, lead), :], halo, halo_sem.at[0], halo_sem.at[1],
            device_id={"tm": z - (1 - (x + edge) // sects), "sect": lax.rem(x + edge, sects)},
            device_id_type=mesh_id)

    def spread(source, half, j):
        def send(i):
            near = i // 2 + 1
            to = lax.rem(x + near + (i % 2) * (sects - 2 * near), sects)
            pltpu.make_async_remote_copy(
                source.at[to], arr_ref.at[half, j, x], row_send.at[half, j], row_recv.at[half, j],
                device_id={"sect": to}, device_id_type=mesh_id).start()

        loop(0, edge, send)
        arr_ref[half, j, x] = source[x]

    def across(half, j):
        pltpu.make_async_remote_copy(
            blk.at[half, j], relay.at[half, z], far_send.at[half, j], far_recv.at[half, z],
            device_id={"tm": j}, device_id_type=mesh_id).start()

    def half_step(half):
        @pl.when(half == 0)
        def _():
            done = x_scr.at[:, :, pl.ds(0, slab), :]
            pltpu.make_async_copy(done, done, load_sem).wait()

        @pl.when(half == 1)
        def _():
            @pl.when(has_next)
            def _():
                pltpu.make_async_copy(halo, halo, halo_sem.at[1]).wait()
                for comp in range(2):
                    for a in range(cols):
                        x_scr[comp, a, pl.ds(slab, lead), :] = halo[comp, :, a * LANES : (a + 1) * LANES]

            @pl.when(jnp.logical_not(has_next))
            def _():
                x_scr[:, :, pl.ds(slab, lead), :] = jnp.zeros((2, cols, lead, LANES), F32)

        coarse_fft(half, rows, x_scr, taps_ref, tw_ref, wh_ref, wl_ref, u_scr, lh_scr, ll_scr, y_scr)

        def put(q, r, vec):
            owner = 4 * q + r
            blk[half, owner // sects, owner % sects] = vec

        order_channels(index_ref, y_scr, z_scr, g_scr, put)

        @pl.when(half == 0)
        def _():
            pl.semaphore_wait(barrier, edge + not_last + wraps)

            @pl.when(z * sects + x > 0)
            def _():
                halo_copy().start()

            @pl.when(z > 0)
            def _():
                pl.semaphore_wait(below, 1)

            @pl.when(z < last)
            def _():
                tell(below, tm=z + 1)
                loop(0, z, lambda j: tell(in_sem.at[z + 1], tm=j))

        loop(0, z, lambda j: across(half, j))
        spread(blk.at[half, z], half, z)

    loop(0, 2, half_step)

    def step(s):
        @pl.when(s < last - z)
        def _():
            @pl.when(s > 0)
            def _():
                pl.semaphore_wait(in_sem.at[z + 1 + s], 1)

            for half in range(2):
                across(half, z + 1 + s)

        @pl.when(s >= LAG)
        def _():
            i = s - LAG
            j = i + (i + tms - z) // tms
            for half in range(2):
                landed = relay.at[half, j]
                pltpu.make_async_copy(landed, landed, far_recv.at[half, j]).wait()
                spread(landed, half, j)

    loop(0, last + LAG, step)

    def finish(j):
        for half in range(2):
            part = arr_ref.at[half, j, pl.ds(0, edge)]
            pltpu.make_async_copy(part, part, row_send.at[half, j]).wait()
            pltpu.make_async_copy(part, part, row_recv.at[half, j]).wait()

            @pl.when(j != z)
            def _():
                sent = blk.at[half, j]
                pltpu.make_async_copy(sent, sent, far_send.at[half, j]).wait()

    loop(0, tms, finish)

    @pl.when(z * sects + x > 0)
    def _():
        pltpu.make_async_copy(halo, halo, halo_sem.at[0]).wait()


def run_front(signal, coarse_taps, index, wh, wl, tw_c, sects, tms):
    slab, width = signal.shape[2:]
    cols = width // LANES
    rows = slab // 2
    vmem = pl.BlockSpec(memory_space=pltpu.VMEM)
    anym = pl.BlockSpec(memory_space=pl.ANY)
    smem = pl.BlockSpec(memory_space=pltpu.SMEM)
    dma = pltpu.SemaphoreType.DMA((2, tms))
    blocks = (2, tms, sects, SUB, LANES)
    return pl.pallas_call(
        front_kernel,
        out_shape=jax.ShapeDtypeStruct(blocks, F32),
        in_specs=[anym, vmem, smem, vmem, vmem, vmem],
        out_specs=vmem,
        scratch_shapes=[
            pltpu.VMEM((2, cols, slab + rows, LANES), F32),
            pltpu.VMEM((2, rows, width), F32),
            pltpu.VMEM((2, cols // 4, 4, rows, LANES), F32),
            pltpu.VMEM((cols * rows, 2 * LANES), BF16),
            pltpu.VMEM((cols * rows, 2 * LANES), BF16),
            pltpu.VMEM((2, cols, rows, LANES), F32),
            pltpu.VMEM((width, LANES), F32),
            pltpu.VMEM((LANES, LANES), F32),
            pltpu.VMEM(blocks, F32),
            pltpu.VMEM(blocks, F32),
            pltpu.SemaphoreType.DMA,
            pltpu.SemaphoreType.DMA((2,)),
            pltpu.SemaphoreType.REGULAR((tms,)),
            pltpu.SemaphoreType.REGULAR,
            dma, dma, dma, dma,
        ],
        compiler_params=pltpu.CompilerParams(collective_id=0, has_side_effects=True),
        name="front",
    )(signal, coarse_taps, index, tw_c, wh, wl)


def tables(width, fine):
    cols, fold = width // LANES, fine // LANES
    wh, wl = dft_matrix(LANES)
    tw_c = twiddles(cols, LANES, width, width ** -0.5)
    tw_f = twiddles(fold, LANES, fine, fine ** -0.5)
    return [jnp.asarray(t) for t in (wh, wl, tw_c, tw_f)]


def run_fine(arrived, taps, wh, wl, tw_f, own, frames, fine):
    vmem = pl.BlockSpec(memory_space=pltpu.VMEM)
    return pl.pallas_call(
        fine_kernel,
        out_shape=jax.ShapeDtypeStruct((2, 1, own, frames, fine), F32),
        in_specs=[vmem] * 5,
        out_specs=vmem,
        scratch_shapes=[
            pltpu.VMEM((2, fine, LANES), F32),
            pltpu.VMEM((2, fine // LANES, LANES, LANES), F32),
        ],
        name="fine",
    )(arrived, taps, tw_f, wh, wl)


def body(signal, coarse_taps, fine_taps, channel_order):
    _, polars, slab, width = signal.shape
    tap_count, fine = fine_taps.shape
    owners = lax.axis_size(("tm", "sect"))
    own = width // owners
    frames = slab * owners // fine
    assert polars == 1 and slab == 4 * SUB and 4 * own == LANES and frames == 4 and tap_count == 16
    wh, wl, tw_c, tw_f = tables(width, fine)
    cols = width // LANES
    index = channel_order % cols * LANES + channel_order // cols
    sects, tms = lax.axis_size("sect"), lax.axis_size("tm")
    assert tap_count - 1 <= slab // 2
    blocks = run_front(signal, coarse_taps, index, wh, wl, tw_c, sects, tms)
    arrived = blocks.reshape(2, owners, SUB, LANES)
    taps = jnp.swapaxes(fine_taps.reshape(tap_count, fine // LANES, LANES), 0, 1)
    return run_fine(arrived, taps, wh, wl, tw_f, own, frames, fine)


def solution(mesh):
    in_specs = (P(None, "pol", ("beam", "tm", "sect"), None), P(), P(), P())
    out_specs = P(None, "pol", ("beam", "tm", "sect"), None, None)
    return jax.shard_map(body, mesh=mesh, in_specs=in_specs, out_specs=out_specs, check_vma=False)
```

```python
from functools import partial
import math

import jax
import jax.numpy as jnp
from jax import lax
from jax.experimental import pallas as pl
from jax.experimental.pallas import tpu as pltpu
from jax.sharding import PartitionSpec as P
import ml_dtypes
import numpy as np

LANES = 128
SUB = 8
F32 = jnp.float32
BF16 = jnp.bfloat16


def split_np(table):
    high = table.astype(ml_dtypes.bfloat16)
    low = (table - high.astype(np.float64)).astype(ml_dtypes.bfloat16)
    return high, low


def dft_matrix(size):
    grid = np.outer(np.arange(size), np.arange(size)) % size
    angle = -2.0 * np.pi * grid / size
    cos, sin = np.cos(angle), np.sin(angle)
    return split_np(np.block([[cos, sin], [-sin, cos]]))


def twiddles(rows, cols, period, scale):
    angle = -2.0 * np.pi * (np.outer(np.arange(rows), np.arange(cols)) % period) / period
    return np.stack([np.cos(angle), np.sin(angle)]).astype(np.float32) * np.float32(scale)


def split(value):
    high = value.astype(BF16)
    return high, (value - high.astype(F32)).astype(BF16)


def times(value, re, im):
    return (value[0] * re - value[1] * im, value[0] * im + value[1] * re)


def add(a, b):
    return (a[0] + b[0], a[1] + b[1])


def sub(a, b):
    return (a[0] - b[0], a[1] - b[1])


def minus_i(a):
    return (a[1], -a[0])


def dft4(x):
    s0, d0, s1, d1 = add(x[0], x[2]), sub(x[0], x[2]), add(x[1], x[3]), minus_i(sub(x[1], x[3]))
    return [add(s0, s1), add(d0, d1), sub(s0, s1), sub(d0, d1)]


def dft8(x):
    half = math.sqrt(0.5)
    even, odd = dft4(x[0::2]), dft4(x[1::2])
    o1, o3 = odd[1], odd[3]
    odd = [
        odd[0],
        ((o1[0] + o1[1]) * half, (o1[1] - o1[0]) * half),
        minus_i(odd[2]),
        ((o3[1] - o3[0]) * half, (o3[0] + o3[1]) * -half),
    ]
    return [add(e, o) for e, o in zip(even, odd)] + [sub(e, o) for e, o in zip(even, odd)]


def group_transpose(vecs, lane):
    size = LANES // 4
    vecs = list(vecs)
    for dist in (1, 2):
        keep = (lane // (size * dist)) % 2 == 0
        for i in range(4):
            if i & dist:
                continue
            a, b = vecs[i], vecs[i + dist]
            vecs[i] = jnp.where(keep, a, pltpu.roll(b, size * dist, 1))
            vecs[i + dist] = jnp.where(keep, pltpu.roll(a, LANES - size * dist, 1), b)
    return vecs


def coarse_fft(half, rows, x_scr, taps_ref, tw_ref, wh_ref, wl_ref, u_scr, lh_scr, ll_scr, y_scr):
    tap_count = taps_ref.shape[0]
    cols = x_scr.shape[1]
    fold = cols // 4
    for r in range(fold):
        parts = []
        for q in range(4):
            a = r + fold * q
            acc = [None, None]
            for k in range(tap_count):
                tap = taps_ref[k : k + 1, a * LANES : (a + 1) * LANES]
                for comp in range(2):
                    term = tap * x_scr[comp, a, pl.ds(half * rows + k, rows, 1), :]
                    acc[comp] = term if k == 0 else acc[comp] + term
            parts.append(tuple(acc))
        for k1, value in enumerate(dft4(parts)):
            if r and k1:
                angle = -2.0 * math.pi * r * k1 / cols
                value = times(value, math.cos(angle), math.sin(angle))
            for comp in range(2):
                u_scr[comp, r, k1] = value[comp]
    for k1 in range(4):
        outs = dft8([(u_scr[0, r, k1], u_scr[1, r, k1]) for r in range(fold)])
        for k2, value in enumerate(outs):
            k = k1 + 4 * k2
            value = times(value, tw_ref[0, k : k + 1, :], tw_ref[1, k : k + 1, :])
            for comp in range(2):
                high, low = split(value[comp])
                lh_scr[pl.ds(k * rows, rows), comp * LANES : (comp + 1) * LANES] = high
                ll_scr[pl.ds(k * rows, rows), comp * LANES : (comp + 1) * LANES] = low
    step = 8 * rows
    for base in range(0, cols * rows, step):
        high, low = lh_scr[base : base + step], ll_scr[base : base + step]
        dot = partial(jnp.dot, preferred_element_type=F32)
        out = dot(high, wh_ref[...]) + (dot(low, wh_ref[...]) + dot(high, wl_ref[...]))
        for comp in range(2):
            piece = out[:, comp * LANES : (comp + 1) * LANES]
            y_scr[comp, base // rows : (base + step) // rows] = piece.reshape(8, rows, LANES)


def order_channels(index_ref, y_scr, z_scr, g_scr, put):
    cols, rows = y_scr.shape[1:3]
    lane = lax.broadcasted_iota(jnp.int32, (SUB, LANES), 1)
    for k in range(cols):
        both = jnp.concatenate([y_scr[0, k], y_scr[1, k]], axis=0)
        z_scr[k * LANES : (k + 1) * LANES, :] = jnp.transpose(jnp.concatenate([both] * 4, axis=0))
    row_lane = lax.broadcasted_iota(jnp.int32, (1, LANES), 1)
    group = LANES // 4
    chunk = 16

    def step(part, carry):
        def fetch(i, inner):
            lists = [index_ref.at[pl.ds((part * 4 + h) * LANES + i * chunk, chunk)] for h in range(4)]
            spot = g_scr.at[pl.ds(pl.multiple_of(i * chunk, chunk), chunk), :]
            for u in range(chunk):
                got = [z_scr[pl.ds(lists[h][u], 1), :] for h in range(4)]
                low = jnp.where(row_lane < group, got[0], got[1])
                high = jnp.where(row_lane < 3 * group, got[2], got[3])
                spot[u : u + 1, :] = jnp.where(row_lane < 2 * group, low, high)
            return inner

        lax.fori_loop(0, LANES // chunk, fetch, 0)
        turned = jnp.transpose(g_scr[...])
        for h in range(4):
            vecs = [turned[(h * 4 + u) * SUB : (h * 4 + u + 1) * SUB] for u in range(4)]
            for r, vec in enumerate(group_transpose(vecs, lane)):
                put(part * 4 + h, r, vec)
        return carry

    lax.fori_loop(0, cols // 4, step, 0)


def fine_fir(arr_ref, taps_ref, xs_scr, frames, per):
    lane = lax.broadcasted_iota(jnp.int32, (SUB, LANES), 1)
    row = lax.broadcasted_iota(jnp.int32, (SUB, LANES), 0)
    slots = LANES // 4
    group = lane // slots
    slab = 4 * SUB

    def step(jb, carry):
        for k4 in range(4):
            jd = jb * 4 + k4
            for half in range(2):
                pick = k4 * slab + half * 2 * SUB + (group % 2) * SUB + row
                taps = [
                    jnp.take_along_axis(
                        jnp.broadcast_to(taps_ref[jb, k : k + 1, :], (SUB, LANES)), pick, axis=1,
                        mode="promise_in_bounds")
                    for k in range(min(frames, taps_ref.shape[1]))
                ]
                data = [arr_ref[half, g * per + jd] for g in range(frames)]
                outs = []
                for f in range(frames):
                    acc = None
                    for k in range(min(frames - f, len(taps))):
                        term = taps[k] * data[f + k]
                        acc = term if acc is None else acc + term
                    outs.append(acc)
                for u, vec in enumerate(group_transpose(outs, lane)):
                    base = pl.multiple_of(jd * slab + half * 2 * SUB + (u % 2) * SUB, SUB)
                    xs_scr[u // 2, pl.ds(base, SUB), :] = vec
        return carry

    lax.fori_loop(0, per // 4, step, 0)


def fine_fft(xs_scr, tw_ref, wh_ref, wl_ref, p_scr, out_ref):
    fold = xs_scr.shape[1] // LANES
    slots, frames = out_ref.shape[2:4]
    dot = partial(jnp.dot, preferred_element_type=F32)
    for a in range(fold):
        pieces = [jnp.transpose(xs_scr[comp, pl.ds(a, LANES, fold), :]) for comp in range(2)]
        high, low = split(jnp.concatenate(pieces, axis=1))
        out = dot(high, wh_ref[...]) + (dot(low, wh_ref[...]) + dot(high, wl_ref[...]))
        value = times((out[:, :LANES], out[:, LANES:]), tw_ref[0, a : a + 1, :], tw_ref[1, a : a + 1, :])
        for comp in range(2):
            for f in range(frames):
                p_scr[comp, a, pl.ds(f, slots, frames), :] = value[comp][f * slots : (f + 1) * slots]
    pack = SUB // frames

    def step(i, carry):
        rows = pl.ds(pl.multiple_of(i * SUB, SUB), SUB)
        outs = dft8([(p_scr[0, a, rows, :], p_scr[1, a, rows, :]) for a in range(fold)])
        for m1, value in enumerate(outs):
            for comp in range(2):
                out_ref[comp, 0, pl.ds(i * pack, pack), :, m1 * LANES : (m1 + 1) * LANES] = value[
                    comp].reshape(pack, frames, LANES)
        return carry

    lax.fori_loop(0, LANES // SUB, step, 0)


def fine_kernel(arr_ref, taps_ref, tw_ref, wh_ref, wl_ref, out_ref, xs_scr, p_scr):
    frames = out_ref.shape[3]
    fine_fir(arr_ref, taps_ref, xs_scr, frames, arr_ref.shape[1] // frames)
    fine_fft(xs_scr, tw_ref, wh_ref, wl_ref, p_scr, out_ref)


EARLY = 5


def front_kernel(sig_ref, taps_ref, index_ref, tw_ref, wh_ref, wl_ref, arr_ref,
                 x_scr, halo, first, second, u_scr, lh_scr, ll_scr, y_scr, z_scr, g_scr, blk, relay,
                 load_sem, halo_sem, leg_sem, in_sem, below, far_send, far_recv, row_send, row_recv):
    slab = sig_ref.shape[2]
    cols = x_scr.shape[1]
    rows = slab // 2
    lead = halo.shape[1]
    tms, sects = blk.shape[1:3]
    x, z = lax.axis_index("sect"), lax.axis_index("tm")
    last, edge = tms - 1, sects - 1
    barrier = pltpu.get_barrier_semaphore()
    mesh_id = pl.DeviceIdType.MESH

    def tell(sem, **where):
        pl.semaphore_signal(sem, inc=1, device_id=where, device_id_type=mesh_id)

    def loop(low, high, step):
        lax.fori_loop(low, high, lambda i, carry: (step(i), carry)[1], 0)

    def load(a):
        lanes = pl.ds(pl.multiple_of(a * LANES, LANES), LANES)
        for comp in range(2):
            pltpu.make_async_copy(
                sig_ref.at[comp, 0, :, lanes], x_scr.at[comp, a, pl.ds(0, slab), :], load_sem).start()

    loop(0, cols, load)

    loop(1, sects, lambda i: tell(barrier, sect=lax.rem(x + i, sects)))

    @pl.when(z > 0)
    def _():
        tell(barrier, tm=z - 1)

    not_last = (last - z + last - 1) // last
    width = halo.shape[2]
    piece = width // sects
    inner, middle = x > 0, x < edge
    lower, upper = z > 0, z < last
    both = jnp.logical_and

    def halo_copy():
        return pltpu.make_async_remote_copy(
            sig_ref.at[:, 0, pl.ds(0, lead), :], halo, halo_sem.at[0], halo_sem.at[1],
            device_id={"sect": x - 1}, device_id_type=mesh_id)

    def to_row(i):
        return pltpu.make_async_remote_copy(
            sig_ref.at[:, 0, pl.ds(0, lead), pl.ds(pl.multiple_of(i * piece, piece), piece)], first,
            leg_sem.at[0], leg_sem.at[1], device_id={"sect": i}, device_id_type=mesh_id)

    def down(source):
        return pltpu.make_async_remote_copy(
            source, second, leg_sem.at[2], leg_sem.at[3], device_id={"tm": z - 1}, device_id_type=mesh_id)

    def to_edge():
        return pltpu.make_async_remote_copy(
            second, halo.at[:, :, pl.ds(pl.multiple_of(x * piece, piece), piece)],
            leg_sem.at[4], halo_sem.at[1], device_id={"sect": edge}, device_id_type=mesh_id)

    def wait_for(part, sem):
        pltpu.make_async_copy(part, part, sem).wait()

    def spread(source, half, j):
        def send(i):
            near = i // 2 + 1
            to = lax.rem(x + near + (i % 2) * (sects - 2 * near), sects)
            pltpu.make_async_remote_copy(
                source.at[to], arr_ref.at[half, j, x], row_send.at[half, j], row_recv.at[half, j],
                device_id={"sect": to}, device_id_type=mesh_id).start()

        loop(0, edge, send)
        arr_ref[half, j, x] = source[x]

    def across(half, j):
        pltpu.make_async_remote_copy(
            blk.at[half, j], relay.at[half, z], far_send.at[half, j], far_recv.at[half, z],
            device_id={"tm": j}, device_id_type=mesh_id).start()

    def half_step(half):
        @pl.when(half == 0)
        def _():
            done = x_scr.at[:, :, pl.ds(0, slab), :]
            pltpu.make_async_copy(done, done, load_sem).wait()
            pl.semaphore_wait(barrier, edge + not_last)

            @pl.when(both(x == 0, lower))
            def _():
                loop(1, sects, lambda i: to_row(sects - i).start())

            @pl.when(inner)
            def _():
                halo_copy().start()

            @pl.when(lower)
            def _():
                pl.semaphore_wait(below, 1)

            @pl.when(z < last)
            def _():
                tell(below, tm=z + 1)
                loop(0, z, lambda j: tell(in_sem.at[z + 1], tm=j))

            @pl.when(both(x == 0, lower))
            def _():
                down(sig_ref.at[:, 0, pl.ds(0, lead), pl.ds(0, piece)]).start()

        @pl.when(half == 1)
        def _():
            @pl.when(middle)
            def _():
                wait_for(halo, halo_sem.at[1])

            @pl.when(both(x == edge, upper))
            def _():
                wait_for(second, leg_sem.at[3])
                wait_for(halo.at[:, :, pl.ds(0, width - piece)], halo_sem.at[1])
                halo[:, :, width - piece :] = second[...]

            @pl.when(jnp.logical_or(middle, upper))
            def _():
                for comp in range(2):
                    for a in range(cols):
                        x_scr[comp, a, pl.ds(slab, lead), :] = halo[comp, :, a * LANES : (a + 1) * LANES]

            @pl.when(both(x == edge, z == last))
            def _():
                x_scr[:, :, pl.ds(slab, lead), :] = jnp.zeros((2, cols, lead, LANES), F32)

        coarse_fft(half, rows, x_scr, taps_ref, tw_ref, wh_ref, wl_ref, u_scr, lh_scr, ll_scr, y_scr)

        def put(q, r, vec):
            owner = 4 * q + r
            blk[half, owner // sects, owner % sects] = vec

        order_channels(index_ref, y_scr, z_scr, g_scr, put)

        @pl.when(both(half == 0, both(inner, lower)))
        def _():
            wait_for(first, leg_sem.at[1])
            down(first).start()

        @pl.when(both(half == 1, both(middle, upper)))
        def _():
            wait_for(second, leg_sem.at[3])
            to_edge().start()

        loop(0, z, lambda j: across(half, j))
        spread(blk.at[half, z], half, z)

        def early(s):
            @pl.when(jnp.logical_and(half == 0, s > 0))
            def _():
                pl.semaphore_wait(in_sem.at[z + 1 + s], 1)

            across(half, z + 1 + s)

        loop(0, jnp.minimum(EARLY, last - z), early)


    loop(0, 2, half_step)

    def later(s):
        pl.semaphore_wait(in_sem.at[z + 1 + s], 1)
        for half in range(2):
            across(half, z + 1 + s)

    loop(EARLY, last - z, later)

    def hand_on(i):
        j = i + (i + tms - z) // tms
        for half in range(2):
            landed = relay.at[half, j]
            pltpu.make_async_copy(landed, landed, far_recv.at[half, j]).wait()
            spread(landed, half, j)

    loop(0, last, hand_on)

    def finish(j):
        for half in range(2):
            part = arr_ref.at[half, j, pl.ds(0, edge)]
            pltpu.make_async_copy(part, part, row_send.at[half, j]).wait()
            pltpu.make_async_copy(part, part, row_recv.at[half, j]).wait()

            @pl.when(j != z)
            def _():
                sent = blk.at[half, j]
                pltpu.make_async_copy(sent, sent, far_send.at[half, j]).wait()

    loop(0, tms, finish)

    @pl.when(inner)
    def _():
        wait_for(halo, halo_sem.at[0])

    @pl.when(both(x == 0, lower))
    def _():
        wait_for(halo.at[:, :, pl.ds(0, width - piece)], leg_sem.at[0])

    @pl.when(lower)
    def _():
        wait_for(second, leg_sem.at[2])

    @pl.when(both(middle, upper))
    def _():
        wait_for(second, leg_sem.at[4])


def run_front(signal, coarse_taps, channel_order, wh, wl, tw_c, sects, tms):
    slab, width = signal.shape[2:]
    cols = width // LANES
    rows = slab // 2
    vmem = pl.BlockSpec(memory_space=pltpu.VMEM)
    anym = pl.BlockSpec(memory_space=pl.ANY)
    smem = pl.BlockSpec(memory_space=pltpu.SMEM)
    dma = pltpu.SemaphoreType.DMA((2, tms))
    blocks = (2, tms, sects, SUB, LANES)
    return pl.pallas_call(
        front_kernel,
        out_shape=jax.ShapeDtypeStruct(blocks, F32),
        in_specs=[anym, vmem, smem, vmem, vmem, vmem],
        out_specs=vmem,
        scratch_shapes=[
            pltpu.VMEM((2, cols, slab + rows, LANES), F32),
            pltpu.VMEM((2, rows, width), F32),
            pltpu.VMEM((2, rows, width // sects), F32),
            pltpu.VMEM((2, rows, width // sects), F32),
            pltpu.VMEM((2, cols // 4, 4, rows, LANES), F32),
            pltpu.VMEM((cols * rows, 2 * LANES), BF16),
            pltpu.VMEM((cols * rows, 2 * LANES), BF16),
            pltpu.VMEM((2, cols, rows, LANES), F32),
            pltpu.VMEM((width, LANES), F32),
            pltpu.VMEM((LANES, LANES), F32),
            pltpu.VMEM(blocks, F32),
            pltpu.VMEM(blocks, F32),
            pltpu.SemaphoreType.DMA,
            pltpu.SemaphoreType.DMA((2,)),
            pltpu.SemaphoreType.DMA((5,)),
            pltpu.SemaphoreType.REGULAR((tms,)),
            pltpu.SemaphoreType.REGULAR,
            dma, dma, dma, dma,
        ],
        compiler_params=pltpu.CompilerParams(collective_id=0, has_side_effects=True),
        name="front",
    )(signal, coarse_taps, channel_order, tw_c, wh, wl)


def tables(width, fine):
    cols, fold = width // LANES, fine // LANES
    wh, wl = dft_matrix(LANES)
    tw_c = twiddles(cols, LANES, width, width ** -0.5)
    tw_f = twiddles(fold, LANES, fine, fine ** -0.5)
    return [jnp.asarray(t) for t in (wh, wl, tw_c, tw_f)]


def run_fine(arrived, taps, wh, wl, tw_f, own, frames, fine):
    vmem = pl.BlockSpec(memory_space=pltpu.VMEM)
    return pl.pallas_call(
        fine_kernel,
        out_shape=jax.ShapeDtypeStruct((2, 1, own, frames, fine), F32),
        in_specs=[vmem] * 5,
        out_specs=vmem,
        scratch_shapes=[
            pltpu.VMEM((2, fine, LANES), F32),
            pltpu.VMEM((2, fine // LANES, LANES, LANES), F32),
        ],
        name="fine",
    )(arrived, taps, tw_f, wh, wl)


def body(signal, coarse_taps, fine_taps, channel_order):
    _, polars, slab, width = signal.shape
    tap_count, fine = fine_taps.shape
    owners = lax.axis_size(("tm", "sect"))
    own = width // owners
    frames = slab * owners // fine
    assert polars == 1 and slab == 4 * SUB and 4 * own == LANES and frames == 4 and tap_count == 16
    wh, wl, tw_c, tw_f = tables(width, fine)
    cols = width // LANES
    index = channel_order % cols * LANES + channel_order // cols
    sects, tms = lax.axis_size("sect"), lax.axis_size("tm")
    assert tap_count - 1 <= slab // 2
    blocks = run_front(signal, coarse_taps, index, wh, wl, tw_c, sects, tms)
    arrived = blocks.reshape(2, owners, SUB, LANES)
    taps = jnp.swapaxes(fine_taps.reshape(tap_count, fine // LANES, LANES), 0, 1)
    return run_fine(arrived, taps, wh, wl, tw_f, own, frames, fine)


def solution(mesh):
    in_specs = (P(None, "pol", ("beam", "tm", "sect"), None), P(), P(), P())
    out_specs = P(None, "pol", ("beam", "tm", "sect"), None, None)
    return jax.shard_map(body, mesh=mesh, in_specs=in_specs, out_specs=out_specs, check_vma=False)
```

```python
from functools import partial
import math

import jax
import jax.numpy as jnp
from jax import lax
from jax.experimental import pallas as pl
from jax.experimental.pallas import tpu as pltpu
from jax.sharding import PartitionSpec as P
import ml_dtypes
import numpy as np

LANES = 128
SUB = 8
F32 = jnp.float32
BF16 = jnp.bfloat16


def split_np(table):
    high = table.astype(ml_dtypes.bfloat16)
    low = (table - high.astype(np.float64)).astype(ml_dtypes.bfloat16)
    return high, low


def dft_matrix(size):
    grid = np.outer(np.arange(size), np.arange(size)) % size
    angle = -2.0 * np.pi * grid / size
    cos, sin = np.cos(angle), np.sin(angle)
    return split_np(np.block([[cos, sin], [-sin, cos]]))


def twiddles(rows, cols, period, scale):
    angle = -2.0 * np.pi * (np.outer(np.arange(rows), np.arange(cols)) % period) / period
    return np.stack([np.cos(angle), np.sin(angle)]).astype(np.float32) * np.float32(scale)


def split(value):
    high = value.astype(BF16)
    return high, (value - high.astype(F32)).astype(BF16)


def times(value, re, im):
    return (value[0] * re - value[1] * im, value[0] * im + value[1] * re)


def add(a, b):
    return (a[0] + b[0], a[1] + b[1])


def sub(a, b):
    return (a[0] - b[0], a[1] - b[1])


def minus_i(a):
    return (a[1], -a[0])


def dft4(x):
    s0, d0, s1, d1 = add(x[0], x[2]), sub(x[0], x[2]), add(x[1], x[3]), minus_i(sub(x[1], x[3]))
    return [add(s0, s1), add(d0, d1), sub(s0, s1), sub(d0, d1)]


def dft8(x):
    half = math.sqrt(0.5)
    even, odd = dft4(x[0::2]), dft4(x[1::2])
    o1, o3 = odd[1], odd[3]
    odd = [
        odd[0],
        ((o1[0] + o1[1]) * half, (o1[1] - o1[0]) * half),
        minus_i(odd[2]),
        ((o3[1] - o3[0]) * half, (o3[0] + o3[1]) * -half),
    ]
    return [add(e, o) for e, o in zip(even, odd)] + [sub(e, o) for e, o in zip(even, odd)]


def group_transpose(vecs, lane):
    size = LANES // 4
    vecs = list(vecs)
    for dist in (1, 2):
        keep = (lane // (size * dist)) % 2 == 0
        for i in range(4):
            if i & dist:
                continue
            a, b = vecs[i], vecs[i + dist]
            vecs[i] = jnp.where(keep, a, pltpu.roll(b, size * dist, 1))
            vecs[i + dist] = jnp.where(keep, pltpu.roll(a, LANES - size * dist, 1), b)
    return vecs


def coarse_fft(half, rows, x_scr, taps_ref, tw_ref, wh_ref, wl_ref, u_scr, lh_scr, ll_scr, y_scr):
    tap_count = taps_ref.shape[0]
    cols = x_scr.shape[1]
    fold = cols // 4
    for r in range(fold):
        parts = []
        for q in range(4):
            a = r + fold * q
            acc = [None, None]
            for k in range(tap_count):
                tap = taps_ref[k : k + 1, a * LANES : (a + 1) * LANES]
                for comp in range(2):
                    term = tap * x_scr[comp, a, pl.ds(half * rows + k, rows, 1), :]
                    acc[comp] = term if k == 0 else acc[comp] + term
            parts.append(tuple(acc))
        for k1, value in enumerate(dft4(parts)):
            if r and k1:
                angle = -2.0 * math.pi * r * k1 / cols
                value = times(value, math.cos(angle), math.sin(angle))
            for comp in range(2):
                u_scr[comp, r, k1] = value[comp]
    for k1 in range(4):
        outs = dft8([(u_scr[0, r, k1], u_scr[1, r, k1]) for r in range(fold)])
        for k2, value in enumerate(outs):
            k = k1 + 4 * k2
            value = times(value, tw_ref[0, k : k + 1, :], tw_ref[1, k : k + 1, :])
            for comp in range(2):
                high, low = split(value[comp])
                lh_scr[pl.ds(k * rows, rows), comp * LANES : (comp + 1) * LANES] = high
                ll_scr[pl.ds(k * rows, rows), comp * LANES : (comp + 1) * LANES] = low
    step = 8 * rows
    for base in range(0, cols * rows, step):
        high, low = lh_scr[base : base + step], ll_scr[base : base + step]
        dot = partial(jnp.dot, preferred_element_type=F32)
        out = dot(high, wh_ref[...]) + (dot(low, wh_ref[...]) + dot(high, wl_ref[...]))
        for comp in range(2):
            piece = out[:, comp * LANES : (comp + 1) * LANES]
            y_scr[comp, base // rows : (base + step) // rows] = piece.reshape(8, rows, LANES)


def order_channels(index_ref, y_scr, z_scr, g_scr, put):
    cols, rows = y_scr.shape[1:3]
    lane = lax.broadcasted_iota(jnp.int32, (SUB, LANES), 1)
    for k in range(cols):
        both = jnp.concatenate([y_scr[0, k], y_scr[1, k]], axis=0)
        z_scr[k * LANES : (k + 1) * LANES, :] = jnp.transpose(jnp.concatenate([both] * 4, axis=0))
    row_lane = lax.broadcasted_iota(jnp.int32, (1, LANES), 1)
    group = LANES // 4
    chunk = 16

    def step(part, carry):
        def fetch(i, inner):
            lists = [index_ref.at[pl.ds((part * 4 + h) * LANES + i * chunk, chunk)] for h in range(4)]
            spot = g_scr.at[pl.ds(pl.multiple_of(i * chunk, chunk), chunk), :]
            for u in range(chunk):
                got = [z_scr[pl.ds(lists[h][u], 1), :] for h in range(4)]
                low = jnp.where(row_lane < group, got[0], got[1])
                high = jnp.where(row_lane < 3 * group, got[2], got[3])
                spot[u : u + 1, :] = jnp.where(row_lane < 2 * group, low, high)
            return inner

        lax.fori_loop(0, LANES // chunk, fetch, 0)
        turned = jnp.transpose(g_scr[...])
        for h in range(4):
            vecs = [turned[(h * 4 + u) * SUB : (h * 4 + u + 1) * SUB] for u in range(4)]
            for r, vec in enumerate(group_transpose(vecs, lane)):
                put(part * 4 + h, r, vec)
        return carry

    lax.fori_loop(0, cols // 4, step, 0)


def fine_fir(arr_ref, taps_ref, xs_scr, frames, per):
    lane = lax.broadcasted_iota(jnp.int32, (SUB, LANES), 1)
    row = lax.broadcasted_iota(jnp.int32, (SUB, LANES), 0)
    slots = LANES // 4
    group = lane // slots
    slab = 4 * SUB

    def step(jb, carry):
        for k4 in range(4):
            jd = jb * 4 + k4
            for half in range(2):
                pick = k4 * slab + half * 2 * SUB + (group % 2) * SUB + row
                taps = [
                    jnp.take_along_axis(
                        jnp.broadcast_to(taps_ref[jb, k : k + 1, :], (SUB, LANES)), pick, axis=1,
                        mode="promise_in_bounds")
                    for k in range(min(frames, taps_ref.shape[1]))
                ]
                data = [arr_ref[half, g * per + jd] for g in range(frames)]
                outs = []
                for f in range(frames):
                    acc = None
                    for k in range(min(frames - f, len(taps))):
                        term = taps[k] * data[f + k]
                        acc = term if acc is None else acc + term
                    outs.append(acc)
                for u, vec in enumerate(group_transpose(outs, lane)):
                    base = pl.multiple_of(jd * slab + half * 2 * SUB + (u % 2) * SUB, SUB)
                    xs_scr[u // 2, pl.ds(base, SUB), :] = vec
        return carry

    lax.fori_loop(0, per // 4, step, 0)


def fine_fft(xs_scr, tw_ref, wh_ref, wl_ref, p_scr, out_ref):
    fold = xs_scr.shape[1] // LANES
    slots, frames = out_ref.shape[2:4]
    dot = partial(jnp.dot, preferred_element_type=F32)
    for a in range(fold):
        pieces = [jnp.transpose(xs_scr[comp, pl.ds(a, LANES, fold), :]) for comp in range(2)]
        high, low = split(jnp.concatenate(pieces, axis=1))
        out = dot(high, wh_ref[...]) + (dot(low, wh_ref[...]) + dot(high, wl_ref[...]))
        value = times((out[:, :LANES], out[:, LANES:]), tw_ref[0, a : a + 1, :], tw_ref[1, a : a + 1, :])
        for comp in range(2):
            for f in range(frames):
                p_scr[comp, a, pl.ds(f, slots, frames), :] = value[comp][f * slots : (f + 1) * slots]
    pack = SUB // frames

    def step(i, carry):
        rows = pl.ds(pl.multiple_of(i * SUB, SUB), SUB)
        outs = dft8([(p_scr[0, a, rows, :], p_scr[1, a, rows, :]) for a in range(fold)])
        for m1, value in enumerate(outs):
            for comp in range(2):
                out_ref[comp, 0, pl.ds(i * pack, pack), :, m1 * LANES : (m1 + 1) * LANES] = value[
                    comp].reshape(pack, frames, LANES)
        return carry

    lax.fori_loop(0, LANES // SUB, step, 0)


def fine_kernel(arr_ref, taps_ref, tw_ref, wh_ref, wl_ref, out_ref, xs_scr, p_scr):
    frames = out_ref.shape[3]
    fine_fir(arr_ref, taps_ref, xs_scr, frames, arr_ref.shape[1] // frames)
    fine_fft(xs_scr, tw_ref, wh_ref, wl_ref, p_scr, out_ref)


EARLY = 4


def front_kernel(sig_ref, taps_ref, index_ref, tw_ref, wh_ref, wl_ref, arr_ref,
                 x_scr, halo, first, second, u_scr, lh_scr, ll_scr, y_scr, z_scr, g_scr, blk, relay,
                 load_sem, halo_sem, leg_sem, in_sem, below, far_send, far_recv, row_send, row_recv):
    slab = sig_ref.shape[2]
    cols = x_scr.shape[1]
    rows = slab // 2
    lead = halo.shape[1]
    tms, sects = blk.shape[1:3]
    x, z = lax.axis_index("sect"), lax.axis_index("tm")
    last, edge = tms - 1, sects - 1
    barrier = pltpu.get_barrier_semaphore()
    mesh_id = pl.DeviceIdType.MESH

    def tell(sem, **where):
        pl.semaphore_signal(sem, inc=1, device_id=where, device_id_type=mesh_id)

    def loop(low, high, step):
        lax.fori_loop(low, high, lambda i, carry: (step(i), carry)[1], 0)

    def load(a):
        lanes = pl.ds(pl.multiple_of(a * LANES, LANES), LANES)
        for comp in range(2):
            pltpu.make_async_copy(
                sig_ref.at[comp, 0, :, lanes], x_scr.at[comp, a, pl.ds(0, slab), :], load_sem).start()

    loop(0, cols, load)

    loop(1, sects, lambda i: tell(barrier, sect=lax.rem(x + i, sects)))

    @pl.when(z > 0)
    def _():
        tell(barrier, tm=z - 1)

    not_last = (last - z + last - 1) // last
    width = halo.shape[2]
    piece = width // sects
    inner, middle = x > 0, x < edge
    lower, upper = z > 0, z < last
    both = jnp.logical_and

    def halo_copy():
        return pltpu.make_async_remote_copy(
            sig_ref.at[:, 0, pl.ds(0, lead), :], halo, halo_sem.at[0], halo_sem.at[1],
            device_id={"sect": x - 1}, device_id_type=mesh_id)

    def to_row(i):
        return pltpu.make_async_remote_copy(
            sig_ref.at[:, 0, pl.ds(0, lead), pl.ds(pl.multiple_of(i * piece, piece), piece)], first,
            leg_sem.at[0], leg_sem.at[1], device_id={"sect": i}, device_id_type=mesh_id)

    def down(source):
        return pltpu.make_async_remote_copy(
            source, second, leg_sem.at[2], leg_sem.at[3], device_id={"tm": z - 1}, device_id_type=mesh_id)

    def first_down():
        down(sig_ref.at[:, 0, pl.ds(0, lead), pl.ds(0, piece)]).start()

    def hand_down():
        @pl.when(inner)
        def _():
            wait_for(first, leg_sem.at[1])
            down(first).start()

    def to_edge():
        return pltpu.make_async_remote_copy(
            second, halo.at[:, :, pl.ds(pl.multiple_of(x * piece, piece), piece)],
            leg_sem.at[4], halo_sem.at[1], device_id={"sect": edge}, device_id_type=mesh_id)

    def wait_for(part, sem):
        pltpu.make_async_copy(part, part, sem).wait()

    def spread(source, half, j):
        def send(i):
            near = i // 2 + 1
            to = lax.rem(x + near + (i % 2) * (sects - 2 * near), sects)
            pltpu.make_async_remote_copy(
                source.at[to], arr_ref.at[half, j, x], row_send.at[half, j], row_recv.at[half, j],
                device_id={"sect": to}, device_id_type=mesh_id).start()

        loop(0, edge, send)
        arr_ref[half, j, x] = source[x]

    def across(half, j):
        pltpu.make_async_remote_copy(
            blk.at[half, j], relay.at[half, z], far_send.at[half, j], far_recv.at[half, z],
            device_id={"tm": j}, device_id_type=mesh_id).start()

    def hear(j):
        pl.semaphore_wait(in_sem.at[j], 1)

        @pl.when(z == 1)
        def _():
            tell(in_sem.at[j], tm=0)

    def half_step(half):
        @pl.when(half == 0)
        def _():
            done = x_scr.at[:, :, pl.ds(0, slab), :]
            pltpu.make_async_copy(done, done, load_sem).wait()
            pl.semaphore_wait(barrier, edge + not_last)

            @pl.when(both(x == 0, lower))
            def _():
                loop(1, sects, lambda i: to_row(sects - i).start())

            @pl.when(inner)
            def _():
                halo_copy().start()

            @pl.when(z > 1)
            def _():
                pl.semaphore_wait(below.at[0], 1)

            @pl.when(z == 0)
            def _():
                tell(below.at[1], tm=z + 1)

            @pl.when(both(lower, upper))
            def _():
                tell(below.at[0], tm=z + 1)
                loop(1, z, lambda j: tell(in_sem.at[z + 1], tm=j))

            @pl.when(both(x == 0, z > 1))
            def _():
                first_down()

        @pl.when(half == 1)
        def _():
            @pl.when(middle)
            def _():
                wait_for(halo, halo_sem.at[1])

            @pl.when(both(x == edge, upper))
            def _():
                wait_for(second, leg_sem.at[3])
                wait_for(halo.at[:, :, pl.ds(0, width - piece)], halo_sem.at[1])
                halo[:, :, width - piece :] = second[...]

            @pl.when(jnp.logical_or(middle, upper))
            def _():
                for comp in range(2):
                    for a in range(cols):
                        x_scr[comp, a, pl.ds(slab, lead), :] = halo[comp, :, a * LANES : (a + 1) * LANES]

            @pl.when(both(x == edge, z == last))
            def _():
                x_scr[:, :, pl.ds(slab, lead), :] = jnp.zeros((2, cols, lead, LANES), F32)

        coarse_fft(half, rows, x_scr, taps_ref, tw_ref, wh_ref, wl_ref, u_scr, lh_scr, ll_scr, y_scr)

        @pl.when(both(half == 1, both(middle, upper)))
        def _():
            wait_for(second, leg_sem.at[3])
            to_edge().start()

        def put(q, r, vec):
            owner = 4 * q + r
            blk[half, owner // sects, owner % sects] = vec

        order_channels(index_ref, y_scr, z_scr, g_scr, put)

        @pl.when(both(half == 0, z > 1))
        def _():
            hand_down()

        @pl.when(both(half == 1, lower))
        def _():
            across(half, 0)

        loop(1, z, lambda j: across(half, j))
        spread(blk.at[half, z], half, z)

        @pl.when(both(half == 0, lower))
        def _():
            pl.semaphore_wait(below.at[1], 1)

            @pl.when(upper)
            def _():
                tell(below.at[1], tm=z + 1)

            @pl.when(z == 1)
            def _():
                tell(in_sem.at[z + 1], tm=0)
                hand_down()

                @pl.when(x == 0)
                def _():
                    first_down()

        @pl.when(both(half == 0, lower))
        def _():
            across(half, 0)

        def early(s):
            @pl.when(jnp.logical_and(half == 0, s > 0))
            def _():
                hear(z + 1 + s)

            across(half, z + 1 + s)

        loop(0, jnp.minimum(EARLY, last - z), early)


    loop(0, 2, half_step)

    def later(s):
        hear(z + 1 + s)
        for half in range(2):
            across(half, z + 1 + s)

    loop(EARLY, last - z, later)

    def hand_on(i):
        j = i + (i + tms - z) // tms
        for half in range(2):
            landed = relay.at[half, j]
            pltpu.make_async_copy(landed, landed, far_recv.at[half, j]).wait()
            spread(landed, half, j)

    loop(0, last, hand_on)

    def finish(j):
        for half in range(2):
            part = arr_ref.at[half, j, pl.ds(0, edge)]
            pltpu.make_async_copy(part, part, row_send.at[half, j]).wait()
            pltpu.make_async_copy(part, part, row_recv.at[half, j]).wait()

            @pl.when(j != z)
            def _():
                sent = blk.at[half, j]
                pltpu.make_async_copy(sent, sent, far_send.at[half, j]).wait()

    loop(0, tms, finish)

    @pl.when(inner)
    def _():
        wait_for(halo, halo_sem.at[0])

    @pl.when(both(x == 0, lower))
    def _():
        wait_for(halo.at[:, :, pl.ds(0, width - piece)], leg_sem.at[0])

    @pl.when(lower)
    def _():
        wait_for(second, leg_sem.at[2])

    @pl.when(both(middle, upper))
    def _():
        wait_for(second, leg_sem.at[4])


def run_front(signal, coarse_taps, channel_order, wh, wl, tw_c, sects, tms):
    slab, width = signal.shape[2:]
    cols = width // LANES
    rows = slab // 2
    vmem = pl.BlockSpec(memory_space=pltpu.VMEM)
    anym = pl.BlockSpec(memory_space=pl.ANY)
    smem = pl.BlockSpec(memory_space=pltpu.SMEM)
    dma = pltpu.SemaphoreType.DMA((2, tms))
    blocks = (2, tms, sects, SUB, LANES)
    return pl.pallas_call(
        front_kernel,
        out_shape=jax.ShapeDtypeStruct(blocks, F32),
        in_specs=[anym, vmem, smem, vmem, vmem, vmem],
        out_specs=vmem,
        scratch_shapes=[
            pltpu.VMEM((2, cols, slab + rows, LANES), F32),
            pltpu.VMEM((2, rows, width), F32),
            pltpu.VMEM((2, rows, width // sects), F32),
            pltpu.VMEM((2, rows, width // sects), F32),
            pltpu.VMEM((2, cols // 4, 4, rows, LANES), F32),
            pltpu.VMEM((cols * rows, 2 * LANES), BF16),
            pltpu.VMEM((cols * rows, 2 * LANES), BF16),
            pltpu.VMEM((2, cols, rows, LANES), F32),
            pltpu.VMEM((width, LANES), F32),
            pltpu.VMEM((LANES, LANES), F32),
            pltpu.VMEM(blocks, F32),
            pltpu.VMEM(blocks, F32),
            pltpu.SemaphoreType.DMA,
            pltpu.SemaphoreType.DMA((2,)),
            pltpu.SemaphoreType.DMA((5,)),
            pltpu.SemaphoreType.REGULAR((tms,)),
            pltpu.SemaphoreType.REGULAR((2,)),
            dma, dma, dma, dma,
        ],
        compiler_params=pltpu.CompilerParams(collective_id=0, has_side_effects=True),
        name="front",
    )(signal, coarse_taps, channel_order, tw_c, wh, wl)


def tables(width, fine):
    cols, fold = width // LANES, fine // LANES
    wh, wl = dft_matrix(LANES)
    tw_c = twiddles(cols, LANES, width, width ** -0.5)
    tw_f = twiddles(fold, LANES, fine, fine ** -0.5)
    return [jnp.asarray(t) for t in (wh, wl, tw_c, tw_f)]


def run_fine(arrived, taps, wh, wl, tw_f, own, frames, fine):
    vmem = pl.BlockSpec(memory_space=pltpu.VMEM)
    return pl.pallas_call(
        fine_kernel,
        out_shape=jax.ShapeDtypeStruct((2, 1, own, frames, fine), F32),
        in_specs=[vmem] * 5,
        out_specs=vmem,
        scratch_shapes=[
            pltpu.VMEM((2, fine, LANES), F32),
            pltpu.VMEM((2, fine // LANES, LANES, LANES), F32),
        ],
        name="fine",
    )(arrived, taps, tw_f, wh, wl)


def body(signal, coarse_taps, fine_taps, channel_order):
    _, polars, slab, width = signal.shape
    tap_count, fine = fine_taps.shape
    owners = lax.axis_size(("tm", "sect"))
    own = width // owners
    frames = slab * owners // fine
    assert polars == 1 and slab == 4 * SUB and 4 * own == LANES and frames == 4 and tap_count == 16
    wh, wl, tw_c, tw_f = tables(width, fine)
    cols = width // LANES
    index = channel_order % cols * LANES + channel_order // cols
    sects, tms = lax.axis_size("sect"), lax.axis_size("tm")
    assert tap_count - 1 <= slab // 2
    blocks = run_front(signal, coarse_taps, index, wh, wl, tw_c, sects, tms)
    arrived = blocks.reshape(2, owners, SUB, LANES)
    taps = jnp.swapaxes(fine_taps.reshape(tap_count, fine // LANES, LANES), 0, 1)
    return run_fine(arrived, taps, wh, wl, tw_f, own, frames, fine)


def solution(mesh):
    in_specs = (P(None, "pol", ("beam", "tm", "sect"), None), P(), P(), P())
    out_specs = P(None, "pol", ("beam", "tm", "sect"), None, None)
    return jax.shard_map(body, mesh=mesh, in_specs=in_specs, out_specs=out_specs, check_vma=False)
```

```python
from functools import partial
import math

import jax
import jax.numpy as jnp
from jax import lax
from jax.experimental import pallas as pl
from jax.experimental.pallas import tpu as pltpu
from jax.sharding import PartitionSpec as P
import ml_dtypes
import numpy as np

LANES = 128
SUB = 8
F32 = jnp.float32
BF16 = jnp.bfloat16


def split_np(table):
    high = table.astype(ml_dtypes.bfloat16)
    low = (table - high.astype(np.float64)).astype(ml_dtypes.bfloat16)
    return high, low


def dft_matrix(size):
    grid = np.outer(np.arange(size), np.arange(size)) % size
    angle = -2.0 * np.pi * grid / size
    cos, sin = np.cos(angle), np.sin(angle)
    return split_np(np.block([[cos, sin], [-sin, cos]]))


def twiddles(rows, cols, period, scale):
    angle = -2.0 * np.pi * (np.outer(np.arange(rows), np.arange(cols)) % period) / period
    return np.stack([np.cos(angle), np.sin(angle)]).astype(np.float32) * np.float32(scale)


def split(value):
    high = value.astype(BF16)
    return high, (value - high.astype(F32)).astype(BF16)


def times(value, re, im):
    return (value[0] * re - value[1] * im, value[0] * im + value[1] * re)


def add(a, b):
    return (a[0] + b[0], a[1] + b[1])


def sub(a, b):
    return (a[0] - b[0], a[1] - b[1])


def minus_i(a):
    return (a[1], -a[0])


def dft4(x):
    s0, d0, s1, d1 = add(x[0], x[2]), sub(x[0], x[2]), add(x[1], x[3]), minus_i(sub(x[1], x[3]))
    return [add(s0, s1), add(d0, d1), sub(s0, s1), sub(d0, d1)]


def dft8(x):
    half = math.sqrt(0.5)
    even, odd = dft4(x[0::2]), dft4(x[1::2])
    o1, o3 = odd[1], odd[3]
    odd = [
        odd[0],
        ((o1[0] + o1[1]) * half, (o1[1] - o1[0]) * half),
        minus_i(odd[2]),
        ((o3[1] - o3[0]) * half, (o3[0] + o3[1]) * -half),
    ]
    return [add(e, o) for e, o in zip(even, odd)] + [sub(e, o) for e, o in zip(even, odd)]


def group_transpose(vecs, lane):
    size = LANES // 4
    group = lane // size
    odd, high = group % 2 == 1, group >= 2
    outer = (group == 0) | (group == 3)

    def pair(a, b):
        turned = pltpu.roll(jnp.where(odd, a, b), size, 1)
        return jnp.where(odd, turned, a), jnp.where(odd, b, turned)

    a, b = pair(vecs[0], vecs[1])
    c, d = pair(vecs[2], vecs[3])
    even = pltpu.roll(jnp.where(high, a, c), 2 * size, 1)
    rest = pltpu.roll(jnp.where(high, b, d), 2 * size, 1)
    kept = jnp.where(high, d, b)
    return [
        jnp.where(high, even, a),
        jnp.where(outer, rest, kept),
        jnp.where(high, c, even),
        jnp.where(outer, kept, rest),
    ]


def coarse_fft(half, rows, x_scr, taps_ref, tw_ref, wh_ref, wl_ref, u_scr, lh_scr, ll_scr, y_scr):
    tap_count = taps_ref.shape[0]
    cols = x_scr.shape[1]
    fold = cols // 4
    for r in range(fold):
        parts = []
        for q in range(4):
            a = r + fold * q
            acc = [None, None]
            for k in range(tap_count):
                tap = taps_ref[k : k + 1, a * LANES : (a + 1) * LANES]
                for comp in range(2):
                    term = tap * x_scr[comp, a, pl.ds(half * rows + k, rows, 1), :]
                    acc[comp] = term if k == 0 else acc[comp] + term
            parts.append(tuple(acc))
        for k1, value in enumerate(dft4(parts)):
            if r and k1:
                angle = -2.0 * math.pi * r * k1 / cols
                value = times(value, math.cos(angle), math.sin(angle))
            for comp in range(2):
                u_scr[comp, r, k1] = value[comp]
    for k1 in range(4):
        outs = dft8([(u_scr[0, r, k1], u_scr[1, r, k1]) for r in range(fold)])
        for k2, value in enumerate(outs):
            k = k1 + 4 * k2
            value = times(value, tw_ref[0, k : k + 1, :], tw_ref[1, k : k + 1, :])
            for comp in range(2):
                high, low = split(value[comp])
                lh_scr[pl.ds(k * rows, rows), comp * LANES : (comp + 1) * LANES] = high
                ll_scr[pl.ds(k * rows, rows), comp * LANES : (comp + 1) * LANES] = low
    step = 8 * rows
    for base in range(0, cols * rows, step):
        high, low = lh_scr[base : base + step], ll_scr[base : base + step]
        dot = partial(jnp.dot, preferred_element_type=F32)
        out = dot(high, wh_ref[...]) + (dot(low, wh_ref[...]) + dot(high, wl_ref[...]))
        for comp in range(2):
            piece = out[:, comp * LANES : (comp + 1) * LANES]
            y_scr[comp, base // rows : (base + step) // rows] = piece.reshape(8, rows, LANES)


def order_channels(index_ref, y_scr, z_scr, g_scr, put):
    cols, rows = y_scr.shape[1:3]
    lane = lax.broadcasted_iota(jnp.int32, (SUB, LANES), 1)
    for k in range(cols):
        both = jnp.concatenate([y_scr[0, k], y_scr[1, k]], axis=0)
        z_scr[k * LANES : (k + 1) * LANES, :] = jnp.transpose(jnp.concatenate([both] * 4, axis=0))
    row_lane = lax.broadcasted_iota(jnp.int32, (1, LANES), 1)
    group = LANES // 4
    chunk = 16
    runs, batch = LANES // chunk, g_scr.shape[0]

    def step(quad, carry):
        def fetch(i, inner):
            part, row = quad * batch + i // runs, i % runs * chunk
            lists = [index_ref.at[pl.ds((part * 4 + h) * LANES + row, chunk)] for h in range(4)]
            spot = g_scr.at[i // runs, pl.ds(pl.multiple_of(row, chunk), chunk), :]
            for u in range(chunk):
                got = [z_scr[pl.ds(lists[h][u], 1), :] for h in range(4)]
                low = jnp.where(row_lane < group, got[0], got[1])
                high = jnp.where(row_lane < 3 * group, got[2], got[3])
                spot[u : u + 1, :] = jnp.where(row_lane < 2 * group, low, high)
            return inner

        lax.fori_loop(0, batch * runs, fetch, 0)
        for p in range(batch):
            turned = jnp.transpose(g_scr[p])
            for h in range(4):
                vecs = [turned[(h * 4 + u) * SUB : (h * 4 + u + 1) * SUB] for u in range(4)]
                for r, vec in enumerate(group_transpose(vecs, lane)):
                    put((quad * batch + p) * 4 + h, r, vec)
        return carry

    lax.fori_loop(0, cols // 4 // batch, step, 0)


def fine_fir(arr_ref, taps_ref, xs_scr, frames, per):
    lane = lax.broadcasted_iota(jnp.int32, (SUB, LANES), 1)
    row = lax.broadcasted_iota(jnp.int32, (SUB, LANES), 0)
    slots = LANES // 4
    group = lane // slots
    slab = 4 * SUB

    def step(jb, carry):
        for k4 in range(4):
            jd = jb * 4 + k4
            for half in range(2):
                pick = k4 * slab + half * 2 * SUB + (group % 2) * SUB + row
                taps = [
                    jnp.take_along_axis(
                        jnp.broadcast_to(taps_ref[jb, k : k + 1, :], (SUB, LANES)), pick, axis=1,
                        mode="promise_in_bounds")
                    for k in range(min(frames, taps_ref.shape[1]))
                ]
                data = [arr_ref[half, g * per + jd] for g in range(frames)]
                outs = []
                for f in range(frames):
                    acc = None
                    for k in range(min(frames - f, len(taps))):
                        term = taps[k] * data[f + k]
                        acc = term if acc is None else acc + term
                    outs.append(acc)
                for u, vec in enumerate(group_transpose(outs, lane)):
                    base = pl.multiple_of(jd * slab + half * 2 * SUB + (u % 2) * SUB, SUB)
                    xs_scr[u // 2, pl.ds(base, SUB), :] = vec
        return carry

    lax.fori_loop(0, per // 4, step, 0, unroll=2)


def fine_fft(xs_scr, tw_ref, wh_ref, wl_ref, p_scr, out_ref):
    fold = xs_scr.shape[1] // LANES
    slots, frames = out_ref.shape[2:4]
    dot = partial(jnp.dot, preferred_element_type=F32)
    for a in range(fold):
        pieces = [jnp.transpose(xs_scr[comp, pl.ds(a, LANES, fold), :]) for comp in range(2)]
        high, low = split(jnp.concatenate(pieces, axis=1))
        out = dot(high, wh_ref[...]) + (dot(low, wh_ref[...]) + dot(high, wl_ref[...]))
        value = times((out[:, :LANES], out[:, LANES:]), tw_ref[0, a : a + 1, :], tw_ref[1, a : a + 1, :])
        for comp in range(2):
            for f in range(frames):
                p_scr[comp, a, pl.ds(f, slots, frames), :] = value[comp][f * slots : (f + 1) * slots]
    pack = SUB // frames

    def step(i, carry):
        rows = pl.ds(pl.multiple_of(i * SUB, SUB), SUB)
        outs = dft8([(p_scr[0, a, rows, :], p_scr[1, a, rows, :]) for a in range(fold)])
        for m1, value in enumerate(outs):
            for comp in range(2):
                out_ref[comp, 0, pl.ds(i * pack, pack), :, m1 * LANES : (m1 + 1) * LANES] = value[
                    comp].reshape(pack, frames, LANES)
        return carry

    lax.fori_loop(0, LANES // SUB, step, 0)


def fine_kernel(arr_ref, taps_ref, tw_ref, wh_ref, wl_ref, out_ref, xs_scr, p_scr):
    frames = out_ref.shape[3]
    fine_fir(arr_ref, taps_ref, xs_scr, frames, arr_ref.shape[1] // frames)
    fine_fft(xs_scr, tw_ref, wh_ref, wl_ref, p_scr, out_ref)


EARLY = 4


def front_kernel(sig_ref, taps_ref, index_ref, tw_ref, wh_ref, wl_ref, arr_ref,
                 x_scr, halo, first, second, u_scr, lh_scr, ll_scr, y_scr, z_scr, g_scr, blk, relay,
                 load_sem, halo_sem, leg_sem, in_sem, below, far_send, far_recv, row_send, row_recv):
    slab = sig_ref.shape[2]
    cols = x_scr.shape[1]
    rows = slab // 2
    lead = halo.shape[1]
    tms, sects = blk.shape[1:3]
    x, z = lax.axis_index("sect"), lax.axis_index("tm")
    last, edge = tms - 1, sects - 1
    barrier = pltpu.get_barrier_semaphore()
    mesh_id = pl.DeviceIdType.MESH

    def tell(sem, **where):
        pl.semaphore_signal(sem, inc=1, device_id=where, device_id_type=mesh_id)

    def loop(low, high, step):
        lax.fori_loop(low, high, lambda i, carry: (step(i), carry)[1], 0)

    def load(a):
        lanes = pl.ds(pl.multiple_of(a * LANES, LANES), LANES)
        for comp in range(2):
            pltpu.make_async_copy(
                sig_ref.at[comp, 0, :, lanes], x_scr.at[comp, a, pl.ds(0, slab), :], load_sem).start()

    loop(0, cols, load)

    loop(1, sects, lambda i: tell(barrier, sect=lax.rem(x + i, sects)))

    @pl.when(z > 0)
    def _():
        tell(barrier, tm=z - 1)

    not_last = (last - z + last - 1) // last
    width = halo.shape[2]
    piece = width // sects
    inner, middle = x > 0, x < edge
    lower, upper = z > 0, z < last
    both = jnp.logical_and

    def halo_copy():
        return pltpu.make_async_remote_copy(
            sig_ref.at[:, 0, pl.ds(0, lead), :], halo, halo_sem.at[0], halo_sem.at[1],
            device_id={"sect": x - 1}, device_id_type=mesh_id)

    def to_row(i):
        return pltpu.make_async_remote_copy(
            sig_ref.at[:, 0, pl.ds(0, lead), pl.ds(pl.multiple_of(i * piece, piece), piece)], first,
            leg_sem.at[0], leg_sem.at[1], device_id={"sect": i}, device_id_type=mesh_id)

    def down(source):
        return pltpu.make_async_remote_copy(
            source, second, leg_sem.at[2], leg_sem.at[3], device_id={"tm": z - 1}, device_id_type=mesh_id)

    def first_down():
        down(sig_ref.at[:, 0, pl.ds(0, lead), pl.ds(0, piece)]).start()

    def hand_down():
        @pl.when(inner)
        def _():
            wait_for(first, leg_sem.at[1])
            down(first).start()

    def to_edge():
        return pltpu.make_async_remote_copy(
            second, halo.at[:, :, pl.ds(pl.multiple_of(x * piece, piece), piece)],
            leg_sem.at[4], halo_sem.at[1], device_id={"sect": edge}, device_id_type=mesh_id)

    def wait_for(part, sem):
        pltpu.make_async_copy(part, part, sem).wait()

    def spread(source, half, j):
        def send(i):
            near = i // 2 + 1
            to = lax.rem(x + near + (i % 2) * (sects - 2 * near), sects)
            pltpu.make_async_remote_copy(
                source.at[to], arr_ref.at[half, j, x], row_send.at[half, j], row_recv.at[half, j],
                device_id={"sect": to}, device_id_type=mesh_id).start()

        loop(0, edge, send)
        arr_ref[half, j, x] = source[x]

    def across(half, j):
        pltpu.make_async_remote_copy(
            blk.at[half, j], relay.at[half, z], far_send.at[half, j], far_recv.at[half, z],
            device_id={"tm": j}, device_id_type=mesh_id).start()

    def hear(j):
        pl.semaphore_wait(in_sem.at[j], 1)

        @pl.when(z == 1)
        def _():
            tell(in_sem.at[j], tm=0)

    def half_step(half):
        @pl.when(half == 0)
        def _():
            done = x_scr.at[:, :, pl.ds(0, slab), :]
            pltpu.make_async_copy(done, done, load_sem).wait()
            pl.semaphore_wait(barrier, edge + not_last)

            @pl.when(both(x == 0, lower))
            def _():
                loop(1, sects, lambda i: to_row(sects - i).start())

            @pl.when(inner)
            def _():
                halo_copy().start()

            @pl.when(z > 1)
            def _():
                pl.semaphore_wait(below.at[0], 1)

            @pl.when(z == 0)
            def _():
                tell(below.at[1], tm=z + 1)

            @pl.when(both(lower, upper))
            def _():
                tell(below.at[0], tm=z + 1)
                loop(1, z, lambda j: tell(in_sem.at[z + 1], tm=j))

            @pl.when(both(x == 0, z > 1))
            def _():
                first_down()

        @pl.when(half == 1)
        def _():
            @pl.when(middle)
            def _():
                wait_for(halo, halo_sem.at[1])

            @pl.when(both(x == edge, upper))
            def _():
                wait_for(second, leg_sem.at[3])
                wait_for(halo.at[:, :, pl.ds(0, width - piece)], halo_sem.at[1])
                halo[:, :, width - piece :] = second[...]

            @pl.when(jnp.logical_or(middle, upper))
            def _():
                for comp in range(2):
                    for a in range(cols):
                        x_scr[comp, a, pl.ds(slab, lead), :] = halo[comp, :, a * LANES : (a + 1) * LANES]

            @pl.when(both(x == edge, z == last))
            def _():
                x_scr[:, :, pl.ds(slab, lead), :] = jnp.zeros((2, cols, lead, LANES), F32)

        coarse_fft(half, rows, x_scr, taps_ref, tw_ref, wh_ref, wl_ref, u_scr, lh_scr, ll_scr, y_scr)

        @pl.when(both(half == 1, both(middle, upper)))
        def _():
            wait_for(second, leg_sem.at[3])
            to_edge().start()

        def put(q, r, vec):
            owner = 4 * q + r
            blk[half, owner // sects, owner % sects] = vec

        order_channels(index_ref, y_scr, z_scr, g_scr, put)

        @pl.when(both(half == 0, z > 1))
        def _():
            hand_down()

        @pl.when(both(half == 1, lower))
        def _():
            across(half, 0)

        loop(1, z, lambda j: across(half, j))
        spread(blk.at[half, z], half, z)

        @pl.when(both(half == 0, lower))
        def _():
            pl.semaphore_wait(below.at[1], 1)

            @pl.when(upper)
            def _():
                tell(below.at[1], tm=z + 1)

            @pl.when(z == 1)
            def _():
                tell(in_sem.at[z + 1], tm=0)
                hand_down()

                @pl.when(x == 0)
                def _():
                    first_down()

        @pl.when(both(half == 0, lower))
        def _():
            across(half, 0)

        def early(s):
            @pl.when(jnp.logical_and(half == 0, s > 0))
            def _():
                hear(z + 1 + s)

            across(half, z + 1 + s)

        loop(0, jnp.minimum(EARLY, last - z), early)


    loop(0, 2, half_step)

    def later(s):
        hear(z + 1 + s)
        for half in range(2):
            across(half, z + 1 + s)

    loop(EARLY, last - z, later)

    def hand_on(i):
        j = i + (i + tms - z) // tms
        for half in range(2):
            landed = relay.at[half, j]
            pltpu.make_async_copy(landed, landed, far_recv.at[half, j]).wait()
            spread(landed, half, j)

    loop(0, last, hand_on)

    def finish(j):
        for half in range(2):
            part = arr_ref.at[half, j, pl.ds(0, edge)]
            pltpu.make_async_copy(part, part, row_send.at[half, j]).wait()
            pltpu.make_async_copy(part, part, row_recv.at[half, j]).wait()

            @pl.when(j != z)
            def _():
                sent = blk.at[half, j]
                pltpu.make_async_copy(sent, sent, far_send.at[half, j]).wait()

    loop(0, tms, finish)

    @pl.when(inner)
    def _():
        wait_for(halo, halo_sem.at[0])

    @pl.when(both(x == 0, lower))
    def _():
        wait_for(halo.at[:, :, pl.ds(0, width - piece)], leg_sem.at[0])

    @pl.when(lower)
    def _():
        wait_for(second, leg_sem.at[2])

    @pl.when(both(middle, upper))
    def _():
        wait_for(second, leg_sem.at[4])


def run_front(signal, coarse_taps, channel_order, wh, wl, tw_c, sects, tms):
    slab, width = signal.shape[2:]
    cols = width // LANES
    rows = slab // 2
    vmem = pl.BlockSpec(memory_space=pltpu.VMEM)
    anym = pl.BlockSpec(memory_space=pl.ANY)
    smem = pl.BlockSpec(memory_space=pltpu.SMEM)
    dma = pltpu.SemaphoreType.DMA((2, tms))
    blocks = (2, tms, sects, SUB, LANES)
    return pl.pallas_call(
        front_kernel,
        out_shape=jax.ShapeDtypeStruct(blocks, F32),
        in_specs=[anym, vmem, smem, vmem, vmem, vmem],
        out_specs=vmem,
        scratch_shapes=[
            pltpu.VMEM((2, cols, slab + rows, LANES), F32),
            pltpu.VMEM((2, rows, width), F32),
            pltpu.VMEM((2, rows, width // sects), F32),
            pltpu.VMEM((2, rows, width // sects), F32),
            pltpu.VMEM((2, cols // 4, 4, rows, LANES), F32),
            pltpu.VMEM((cols * rows, 2 * LANES), BF16),
            pltpu.VMEM((cols * rows, 2 * LANES), BF16),
            pltpu.VMEM((2, cols, rows, LANES), F32),
            pltpu.VMEM((width, LANES), F32),
            pltpu.VMEM((4, LANES, LANES), F32),
            pltpu.VMEM(blocks, F32),
            pltpu.VMEM(blocks, F32),
            pltpu.SemaphoreType.DMA,
            pltpu.SemaphoreType.DMA((2,)),
            pltpu.SemaphoreType.DMA((5,)),
            pltpu.SemaphoreType.REGULAR((tms,)),
            pltpu.SemaphoreType.REGULAR((2,)),
            dma, dma, dma, dma,
        ],
        compiler_params=pltpu.CompilerParams(collective_id=0, has_side_effects=True),
        name="front",
    )(signal, coarse_taps, channel_order, tw_c, wh, wl)


def tables(width, fine):
    cols, fold = width // LANES, fine // LANES
    wh, wl = dft_matrix(LANES)
    tw_c = twiddles(cols, LANES, width, width ** -0.5)
    tw_f = twiddles(fold, LANES, fine, fine ** -0.5)
    return [jnp.asarray(t) for t in (wh, wl, tw_c, tw_f)]


def run_fine(arrived, taps, wh, wl, tw_f, own, frames, fine):
    vmem = pl.BlockSpec(memory_space=pltpu.VMEM)
    return pl.pallas_call(
        fine_kernel,
        out_shape=jax.ShapeDtypeStruct((2, 1, own, frames, fine), F32),
        in_specs=[vmem] * 5,
        out_specs=vmem,
        scratch_shapes=[
            pltpu.VMEM((2, fine, LANES), F32),
            pltpu.VMEM((2, fine // LANES, LANES, LANES), F32),
        ],
        name="fine",
    )(arrived, taps, tw_f, wh, wl)


def body(signal, coarse_taps, fine_taps, channel_order):
    _, polars, slab, width = signal.shape
    tap_count, fine = fine_taps.shape
    owners = lax.axis_size(("tm", "sect"))
    own = width // owners
    frames = slab * owners // fine
    assert polars == 1 and slab == 4 * SUB and 4 * own == LANES and frames == 4 and tap_count == 16
    wh, wl, tw_c, tw_f = tables(width, fine)
    cols = width // LANES
    index = channel_order % cols * LANES + channel_order // cols
    sects, tms = lax.axis_size("sect"), lax.axis_size("tm")
    assert tap_count - 1 <= slab // 2
    blocks = run_front(signal, coarse_taps, index, wh, wl, tw_c, sects, tms)
    arrived = blocks.reshape(2, owners, SUB, LANES)
    taps = jnp.swapaxes(fine_taps.reshape(tap_count, fine // LANES, LANES), 0, 1)
    return run_fine(arrived, taps, wh, wl, tw_f, own, frames, fine)


def solution(mesh):
    in_specs = (P(None, "pol", ("beam", "tm", "sect"), None), P(), P(), P())
    out_specs = P(None, "pol", ("beam", "tm", "sect"), None, None)
    return jax.shard_map(body, mesh=mesh, in_specs=in_specs, out_specs=out_specs, check_vma=False)
```

```python
from functools import partial
import math

import jax
import jax.numpy as jnp
from jax import lax
from jax.experimental import pallas as pl
from jax.experimental.pallas import tpu as pltpu
from jax.sharding import PartitionSpec as P
import ml_dtypes
import numpy as np

LANES = 128
SUB = 8
F32 = jnp.float32
BF16 = jnp.bfloat16


def split_np(table):
    high = table.astype(ml_dtypes.bfloat16)
    low = (table - high.astype(np.float64)).astype(ml_dtypes.bfloat16)
    return high, low


def dft_matrix(size):
    grid = np.outer(np.arange(size), np.arange(size)) % size
    angle = -2.0 * np.pi * grid / size
    cos, sin = np.cos(angle), np.sin(angle)
    return split_np(np.block([[cos, sin], [-sin, cos]]))


def twiddles(rows, cols, period, scale):
    angle = -2.0 * np.pi * (np.outer(np.arange(rows), np.arange(cols)) % period) / period
    return np.stack([np.cos(angle), np.sin(angle)]).astype(np.float32) * np.float32(scale)


def split(value):
    high = value.astype(BF16)
    return high, (value - high.astype(F32)).astype(BF16)


def times(value, re, im):
    return (value[0] * re - value[1] * im, value[0] * im + value[1] * re)


def add(a, b):
    return (a[0] + b[0], a[1] + b[1])


def sub(a, b):
    return (a[0] - b[0], a[1] - b[1])


def minus_i(a):
    return (a[1], -a[0])


def dft4(x):
    s0, d0, s1, d1 = add(x[0], x[2]), sub(x[0], x[2]), add(x[1], x[3]), minus_i(sub(x[1], x[3]))
    return [add(s0, s1), add(d0, d1), sub(s0, s1), sub(d0, d1)]


def dft8(x):
    half = math.sqrt(0.5)
    even, odd = dft4(x[0::2]), dft4(x[1::2])
    o1, o3 = odd[1], odd[3]
    odd = [
        odd[0],
        ((o1[0] + o1[1]) * half, (o1[1] - o1[0]) * half),
        minus_i(odd[2]),
        ((o3[1] - o3[0]) * half, (o3[0] + o3[1]) * -half),
    ]
    return [add(e, o) for e, o in zip(even, odd)] + [sub(e, o) for e, o in zip(even, odd)]


def group_transpose(vecs, lane):
    size = LANES // 4
    group = lane // size
    odd, high = group % 2 == 1, group >= 2
    outer = (group == 0) | (group == 3)

    def pair(a, b):
        turned = pltpu.roll(jnp.where(odd, a, b), size, 1)
        return jnp.where(odd, turned, a), jnp.where(odd, b, turned)

    a, b = pair(vecs[0], vecs[1])
    c, d = pair(vecs[2], vecs[3])
    even = pltpu.roll(jnp.where(high, a, c), 2 * size, 1)
    rest = pltpu.roll(jnp.where(high, b, d), 2 * size, 1)
    kept = jnp.where(high, d, b)
    return [
        jnp.where(high, even, a),
        jnp.where(outer, rest, kept),
        jnp.where(high, c, even),
        jnp.where(outer, kept, rest),
    ]


def coarse_fft(half, rows, x_scr, taps_ref, tw_ref, wh_ref, wl_ref, u_scr, lh_scr, ll_scr, y_scr):
    tap_count = taps_ref.shape[0]
    cols = x_scr.shape[1]
    fold = cols // 4
    for r in range(fold):
        parts = []
        for q in range(4):
            a = r + fold * q
            acc = [None, None]
            for k in range(tap_count):
                tap = taps_ref[k : k + 1, a * LANES : (a + 1) * LANES]
                for comp in range(2):
                    term = tap * x_scr[comp, a, pl.ds(half * rows + k, rows, 1), :]
                    acc[comp] = term if k == 0 else acc[comp] + term
            parts.append(tuple(acc))
        for k1, value in enumerate(dft4(parts)):
            if r and k1:
                angle = -2.0 * math.pi * r * k1 / cols
                value = times(value, math.cos(angle), math.sin(angle))
            for comp in range(2):
                u_scr[comp, r, k1] = value[comp]
    for k1 in range(4):
        outs = dft8([(u_scr[0, r, k1], u_scr[1, r, k1]) for r in range(fold)])
        for k2, value in enumerate(outs):
            k = k1 + 4 * k2
            value = times(value, tw_ref[0, k : k + 1, :], tw_ref[1, k : k + 1, :])
            for comp in range(2):
                high, low = split(value[comp])
                lh_scr[pl.ds(k * rows, rows), comp * LANES : (comp + 1) * LANES] = high
                ll_scr[pl.ds(k * rows, rows), comp * LANES : (comp + 1) * LANES] = low
    step = 8 * rows
    for base in range(0, cols * rows, step):
        high, low = lh_scr[base : base + step], ll_scr[base : base + step]
        dot = partial(jnp.dot, preferred_element_type=F32)
        out = dot(high, wh_ref[...]) + (dot(low, wh_ref[...]) + dot(high, wl_ref[...]))
        for comp in range(2):
            piece = out[:, comp * LANES : (comp + 1) * LANES]
            y_scr[comp, base // rows : (base + step) // rows] = piece.reshape(8, rows, LANES)


def order_channels(index_ref, y_scr, z_scr, g_scr, put):
    cols, rows = y_scr.shape[1:3]
    lane = lax.broadcasted_iota(jnp.int32, (SUB, LANES), 1)
    for k in range(cols):
        both = jnp.concatenate([y_scr[0, k], y_scr[1, k]], axis=0)
        z_scr[k * LANES : (k + 1) * LANES, :] = jnp.transpose(jnp.concatenate([both] * 4, axis=0))
    row_lane = lax.broadcasted_iota(jnp.int32, (1, LANES), 1)
    group = LANES // 4
    chunk = 16
    runs, batch = LANES // chunk, g_scr.shape[0]

    def step(quad, carry):
        def fetch(i, inner):
            part, row = quad * batch + i // runs, i % runs * chunk
            lists = [index_ref.at[pl.ds((part * 4 + h) * LANES + row, chunk)] for h in range(4)]
            spot = g_scr.at[i // runs, pl.ds(pl.multiple_of(row, chunk), chunk), :]
            for u in range(chunk):
                got = [z_scr[pl.ds(lists[h][u], 1), :] for h in range(4)]
                low = jnp.where(row_lane < group, got[0], got[1])
                high = jnp.where(row_lane < 3 * group, got[2], got[3])
                spot[u : u + 1, :] = jnp.where(row_lane < 2 * group, low, high)
            return inner

        lax.fori_loop(0, batch * runs, fetch, 0)
        for p in range(batch):
            turned = jnp.transpose(g_scr[p])
            for h in range(4):
                vecs = [turned[(h * 4 + u) * SUB : (h * 4 + u + 1) * SUB] for u in range(4)]
                for r, vec in enumerate(group_transpose(vecs, lane)):
                    put((quad * batch + p) * 4 + h, r, vec)
        return carry

    lax.fori_loop(0, cols // 4 // batch, step, 0)


def fine_fir(arr_ref, taps_ref, xs_scr, frames, per):
    lane = lax.broadcasted_iota(jnp.int32, (SUB, LANES), 1)
    row = lax.broadcasted_iota(jnp.int32, (SUB, LANES), 0)
    slots = LANES // 4
    group = lane // slots
    slab = 4 * SUB

    def step(jb, carry):
        for k4 in range(4):
            jd = jb * 4 + k4
            for half in range(2):
                pick = k4 * slab + half * 2 * SUB + (group % 2) * SUB + row
                taps = [
                    jnp.take_along_axis(
                        jnp.broadcast_to(taps_ref[jb, k : k + 1, :], (SUB, LANES)), pick, axis=1,
                        mode="promise_in_bounds")
                    for k in range(min(frames, taps_ref.shape[1]))
                ]
                data = [arr_ref[half, g * per + jd] for g in range(frames)]
                outs = []
                for f in range(frames):
                    acc = None
                    for k in range(min(frames - f, len(taps))):
                        term = taps[k] * data[f + k]
                        acc = term if acc is None else acc + term
                    outs.append(acc)
                for u, vec in enumerate(group_transpose(outs, lane)):
                    base = pl.multiple_of(jd * slab + half * 2 * SUB + (u % 2) * SUB, SUB)
                    xs_scr[u // 2, pl.ds(base, SUB), :] = vec
        return carry

    lax.fori_loop(0, per // 4, step, 0, unroll=4)


def fine_fft(xs_scr, tw_ref, wh_ref, wl_ref, p_scr, out_ref):
    fold = xs_scr.shape[1] // LANES
    slots, frames = out_ref.shape[2:4]
    dot = partial(jnp.dot, preferred_element_type=F32)
    for a in range(fold):
        pieces = [jnp.transpose(xs_scr[comp, pl.ds(a, LANES, fold), :]) for comp in range(2)]
        high, low = split(jnp.concatenate(pieces, axis=1))
        out = dot(high, wh_ref[...]) + (dot(low, wh_ref[...]) + dot(high, wl_ref[...]))
        value = times((out[:, :LANES], out[:, LANES:]), tw_ref[0, a : a + 1, :], tw_ref[1, a : a + 1, :])
        for comp in range(2):
            for f in range(frames):
                p_scr[comp, a, pl.ds(f, slots, frames), :] = value[comp][f * slots : (f + 1) * slots]
    pack = SUB // frames

    def step(i, carry):
        rows = pl.ds(pl.multiple_of(i * SUB, SUB), SUB)
        outs = dft8([(p_scr[0, a, rows, :], p_scr[1, a, rows, :]) for a in range(fold)])
        for m1, value in enumerate(outs):
            for comp in range(2):
                out_ref[comp, 0, pl.ds(i * pack, pack), :, m1 * LANES : (m1 + 1) * LANES] = value[
                    comp].reshape(pack, frames, LANES)
        return carry

    lax.fori_loop(0, LANES // SUB, step, 0, unroll=2)


def fine_kernel(arr_ref, taps_ref, tw_ref, wh_ref, wl_ref, out_ref, xs_scr, p_scr):
    frames = out_ref.shape[3]
    fine_fir(arr_ref, taps_ref, xs_scr, frames, arr_ref.shape[1] // frames)
    fine_fft(xs_scr, tw_ref, wh_ref, wl_ref, p_scr, out_ref)


EARLY = 4


def front_kernel(sig_ref, taps_ref, index_ref, tw_ref, wh_ref, wl_ref, arr_ref,
                 x_scr, halo, first, second, u_scr, lh_scr, ll_scr, y_scr, z_scr, g_scr, blk, relay,
                 load_sem, halo_sem, leg_sem, in_sem, below, far_send, far_recv, row_send, row_recv):
    slab = sig_ref.shape[2]
    cols = x_scr.shape[1]
    rows = slab // 2
    lead = halo.shape[1]
    tms, sects = blk.shape[1:3]
    x, z = lax.axis_index("sect"), lax.axis_index("tm")
    last, edge = tms - 1, sects - 1
    barrier = pltpu.get_barrier_semaphore()
    mesh_id = pl.DeviceIdType.MESH

    def tell(sem, **where):
        pl.semaphore_signal(sem, inc=1, device_id=where, device_id_type=mesh_id)

    def loop(low, high, step):
        lax.fori_loop(low, high, lambda i, carry: (step(i), carry)[1], 0)

    def load(a):
        lanes = pl.ds(pl.multiple_of(a * LANES, LANES), LANES)
        for comp in range(2):
            pltpu.make_async_copy(
                sig_ref.at[comp, 0, :, lanes], x_scr.at[comp, a, pl.ds(0, slab), :], load_sem).start()

    loop(0, cols, load)

    loop(1, sects, lambda i: tell(barrier, sect=lax.rem(x + i, sects)))

    @pl.when(z > 0)
    def _():
        tell(barrier, tm=z - 1)

    not_last = (last - z + last - 1) // last
    width = halo.shape[2]
    piece = width // sects
    inner, middle = x > 0, x < edge
    lower, upper = z > 0, z < last
    both = jnp.logical_and

    def halo_copy():
        return pltpu.make_async_remote_copy(
            sig_ref.at[:, 0, pl.ds(0, lead), :], halo, halo_sem.at[0], halo_sem.at[1],
            device_id={"sect": x - 1}, device_id_type=mesh_id)

    def to_row(i):
        return pltpu.make_async_remote_copy(
            sig_ref.at[:, 0, pl.ds(0, lead), pl.ds(pl.multiple_of(i * piece, piece), piece)], first,
            leg_sem.at[0], leg_sem.at[1], device_id={"sect": i}, device_id_type=mesh_id)

    def down(source):
        return pltpu.make_async_remote_copy(
            source, second, leg_sem.at[2], leg_sem.at[3], device_id={"tm": z - 1}, device_id_type=mesh_id)

    def first_down():
        down(sig_ref.at[:, 0, pl.ds(0, lead), pl.ds(0, piece)]).start()

    def hand_down():
        @pl.when(inner)
        def _():
            wait_for(first, leg_sem.at[1])
            down(first).start()

    def to_edge():
        return pltpu.make_async_remote_copy(
            second, halo.at[:, :, pl.ds(pl.multiple_of(x * piece, piece), piece)],
            leg_sem.at[4], halo_sem.at[1], device_id={"sect": edge}, device_id_type=mesh_id)

    def wait_for(part, sem):
        pltpu.make_async_copy(part, part, sem).wait()

    def spread(source, half, j):
        def send(i):
            near = i // 2 + 1
            to = lax.rem(x + near + (i % 2) * (sects - 2 * near), sects)
            pltpu.make_async_remote_copy(
                source.at[to], arr_ref.at[half, j, x], row_send.at[half, j], row_recv.at[half, j],
                device_id={"sect": to}, device_id_type=mesh_id).start()

        loop(0, edge, send)
        arr_ref[half, j, x] = source[x]

    def across(half, j):
        pltpu.make_async_remote_copy(
            blk.at[half, j], relay.at[half, z], far_send.at[half, j], far_recv.at[half, z],
            device_id={"tm": j}, device_id_type=mesh_id).start()

    def hear(j):
        pl.semaphore_wait(in_sem.at[j], 1)

        @pl.when(z == 1)
        def _():
            tell(in_sem.at[j], tm=0)

    def half_step(half):
        @pl.when(half == 0)
        def _():
            done = x_scr.at[:, :, pl.ds(0, slab), :]
            pltpu.make_async_copy(done, done, load_sem).wait()
            pl.semaphore_wait(barrier, edge + not_last)

            @pl.when(both(x == 0, lower))
            def _():
                loop(1, sects, lambda i: to_row(sects - i).start())

            @pl.when(inner)
            def _():
                halo_copy().start()

            @pl.when(z > 1)
            def _():
                pl.semaphore_wait(below.at[0], 1)

            @pl.when(z == 0)
            def _():
                tell(below.at[1], tm=z + 1)

            @pl.when(both(lower, upper))
            def _():
                tell(below.at[0], tm=z + 1)
                loop(1, z, lambda j: tell(in_sem.at[z + 1], tm=j))

            @pl.when(both(x == 0, z > 1))
            def _():
                first_down()

        @pl.when(half == 1)
        def _():
            @pl.when(middle)
            def _():
                wait_for(halo, halo_sem.at[1])

            @pl.when(both(x == edge, upper))
            def _():
                wait_for(second, leg_sem.at[3])
                wait_for(halo.at[:, :, pl.ds(0, width - piece)], halo_sem.at[1])
                halo[:, :, width - piece :] = second[...]

            @pl.when(jnp.logical_or(middle, upper))
            def _():
                for comp in range(2):
                    for a in range(cols):
                        x_scr[comp, a, pl.ds(slab, lead), :] = halo[comp, :, a * LANES : (a + 1) * LANES]

            @pl.when(both(x == edge, z == last))
            def _():
                x_scr[:, :, pl.ds(slab, lead), :] = jnp.zeros((2, cols, lead, LANES), F32)

        coarse_fft(half, rows, x_scr, taps_ref, tw_ref, wh_ref, wl_ref, u_scr, lh_scr, ll_scr, y_scr)

        @pl.when(both(half == 1, both(middle, upper)))
        def _():
            wait_for(second, leg_sem.at[3])
            to_edge().start()

        def put(q, r, vec):
            owner = 4 * q + r
            blk[half, owner // sects, owner % sects] = vec

        order_channels(index_ref, y_scr, z_scr, g_scr, put)

        @pl.when(both(half == 0, z > 1))
        def _():
            hand_down()

        @pl.when(both(half == 1, lower))
        def _():
            across(half, 0)

        loop(1, z, lambda j: across(half, j))
        spread(blk.at[half, z], half, z)

        @pl.when(both(half == 0, lower))
        def _():
            pl.semaphore_wait(below.at[1], 1)

            @pl.when(upper)
            def _():
                tell(below.at[1], tm=z + 1)

            @pl.when(z == 1)
            def _():
                tell(in_sem.at[z + 1], tm=0)
                hand_down()

                @pl.when(x == 0)
                def _():
                    first_down()

        @pl.when(both(half == 0, lower))
        def _():
            across(half, 0)

        def early(s):
            @pl.when(jnp.logical_and(half == 0, s > 0))
            def _():
                hear(z + 1 + s)

            across(half, z + 1 + s)

        loop(0, jnp.minimum(EARLY, last - z), early)


    loop(0, 2, half_step)

    def later(s):
        hear(z + 1 + s)
        for half in range(2):
            across(half, z + 1 + s)

    loop(EARLY, last - z, later)

    def hand_on(i):
        j = i + (i + tms - z) // tms
        for half in range(2):
            landed = relay.at[half, j]
            pltpu.make_async_copy(landed, landed, far_recv.at[half, j]).wait()
            spread(landed, half, j)

    loop(0, last, hand_on)

    def finish(j):
        for half in range(2):
            part = arr_ref.at[half, j, pl.ds(0, edge)]
            pltpu.make_async_copy(part, part, row_send.at[half, j]).wait()
            pltpu.make_async_copy(part, part, row_recv.at[half, j]).wait()

            @pl.when(j != z)
            def _():
                sent = blk.at[half, j]
                pltpu.make_async_copy(sent, sent, far_send.at[half, j]).wait()

    loop(0, tms, finish)

    @pl.when(inner)
    def _():
        wait_for(halo, halo_sem.at[0])

    @pl.when(both(x == 0, lower))
    def _():
        wait_for(halo.at[:, :, pl.ds(0, width - piece)], leg_sem.at[0])

    @pl.when(lower)
    def _():
        wait_for(second, leg_sem.at[2])

    @pl.when(both(middle, upper))
    def _():
        wait_for(second, leg_sem.at[4])


def run_front(signal, coarse_taps, channel_order, wh, wl, tw_c, sects, tms):
    slab, width = signal.shape[2:]
    cols = width // LANES
    rows = slab // 2
    vmem = pl.BlockSpec(memory_space=pltpu.VMEM)
    anym = pl.BlockSpec(memory_space=pl.ANY)
    smem = pl.BlockSpec(memory_space=pltpu.SMEM)
    dma = pltpu.SemaphoreType.DMA((2, tms))
    blocks = (2, tms, sects, SUB, LANES)
    return pl.pallas_call(
        front_kernel,
        out_shape=jax.ShapeDtypeStruct(blocks, F32),
        in_specs=[anym, vmem, smem, vmem, vmem, vmem],
        out_specs=vmem,
        scratch_shapes=[
            pltpu.VMEM((2, cols, slab + rows, LANES), F32),
            pltpu.VMEM((2, rows, width), F32),
            pltpu.VMEM((2, rows, width // sects), F32),
            pltpu.VMEM((2, rows, width // sects), F32),
            pltpu.VMEM((2, cols // 4, 4, rows, LANES), F32),
            pltpu.VMEM((cols * rows, 2 * LANES), BF16),
            pltpu.VMEM((cols * rows, 2 * LANES), BF16),
            pltpu.VMEM((2, cols, rows, LANES), F32),
            pltpu.VMEM((width, LANES), F32),
            pltpu.VMEM((4, LANES, LANES), F32),
            pltpu.VMEM(blocks, F32),
            pltpu.VMEM(blocks, F32),
            pltpu.SemaphoreType.DMA,
            pltpu.SemaphoreType.DMA((2,)),
            pltpu.SemaphoreType.DMA((5,)),
            pltpu.SemaphoreType.REGULAR((tms,)),
            pltpu.SemaphoreType.REGULAR((2,)),
            dma, dma, dma, dma,
        ],
        compiler_params=pltpu.CompilerParams(collective_id=0, has_side_effects=True),
        name="front",
    )(signal, coarse_taps, channel_order, tw_c, wh, wl)


def tables(width, fine):
    cols, fold = width // LANES, fine // LANES
    wh, wl = dft_matrix(LANES)
    tw_c = twiddles(cols, LANES, width, width ** -0.5)
    tw_f = twiddles(fold, LANES, fine, fine ** -0.5)
    return [jnp.asarray(t) for t in (wh, wl, tw_c, tw_f)]


def run_fine(arrived, taps, wh, wl, tw_f, own, frames, fine):
    vmem = pl.BlockSpec(memory_space=pltpu.VMEM)
    return pl.pallas_call(
        fine_kernel,
        out_shape=jax.ShapeDtypeStruct((2, 1, own, frames, fine), F32),
        in_specs=[vmem] * 5,
        out_specs=vmem,
        scratch_shapes=[
            pltpu.VMEM((2, fine, LANES), F32),
            pltpu.VMEM((2, fine // LANES, LANES, LANES), F32),
        ],
        name="fine",
    )(arrived, taps, tw_f, wh, wl)


def body(signal, coarse_taps, fine_taps, channel_order):
    _, polars, slab, width = signal.shape
    tap_count, fine = fine_taps.shape
    owners = lax.axis_size(("tm", "sect"))
    own = width // owners
    frames = slab * owners // fine
    assert polars == 1 and slab == 4 * SUB and 4 * own == LANES and frames == 4 and tap_count == 16
    wh, wl, tw_c, tw_f = tables(width, fine)
    cols = width // LANES
    index = channel_order % cols * LANES + channel_order // cols
    sects, tms = lax.axis_size("sect"), lax.axis_size("tm")
    assert tap_count - 1 <= slab // 2
    blocks = run_front(signal, coarse_taps, index, wh, wl, tw_c, sects, tms)
    arrived = blocks.reshape(2, owners, SUB, LANES)
    taps = jnp.swapaxes(fine_taps.reshape(tap_count, fine // LANES, LANES), 0, 1)
    return run_fine(arrived, taps, wh, wl, tw_f, own, frames, fine)


def solution(mesh):
    in_specs = (P(None, "pol", ("beam", "tm", "sect"), None), P(), P(), P())
    out_specs = P(None, "pol", ("beam", "tm", "sect"), None, None)
    return jax.shard_map(body, mesh=mesh, in_specs=in_specs, out_specs=out_specs, check_vma=False)
```
